32 devices in a mesh: mem: 8 (over y, x, core), pix: 4 (over z).
Axes of the slice: x: 2, y: 2, z: 4, core: 2. Of those that a mesh axis runs over, the one named last changes fastest.
Arguments:
- prior_motion: bfloat16 [64, 16, 131072], P('mem', None, 'pix'), may hold values from -6 to 6
- measured_motion: float32 [1200], replicated, may hold values from -1.6 to 1.6
- measurement_noise_stddev: float32 [1200], replicated, may hold values from 0.05 to 0.5
- gaussian_jitter: float32 [2, 1200, 64], replicated, may hold values from -6 to 6
- scene_couples: int32 [2, 1200], replicated, may hold values from 0 to 15, as said below
- targeted_tile_number: int32 [1200], replicated, may hold values from 0 to 2047
Outputs:
- analysis: bfloat16 [64, 16, 131072], P('mem', None, 'pix')
The draws below stay inside these ranges and needn't reach their ends.
Inputs may be any that keep to these rules, and one draw needn't show every extreme that they name: scene_couples[0, k] < scene_couples[1, k]: row 0 holds the earlier acquisition, row 1 the later.
All inputs are finite; a program needn't handle non-finite values.
Results may differ from the reference program's by a relative error of at most 0.011.
Values may be sent and summed in bfloat16 or wider, within the bound.
A program may use at most 192 MiB of HBM per device.

```python
import math
import jax
import jax.numpy as jnp
from jax import lax

REALIZATION_NUM = 64
SCENE_TIMES = 16
NOBS = 1200
BLK = 64
PASS_COUNT = 2
RASTER_CELLS = 131072
NBLK = 2048
N_MEM = 8
N_PIX = 4


def draw_scene_couples(key, part):
    key_first = jax.random.fold_in(key, 11)
    key_gap = jax.random.fold_in(key, 12)
    earlier = jax.random.randint(key_first, (NOBS,), 0, SCENE_TIMES - 1)
    offset = jax.random.randint(key_gap, (NOBS,), 0, SCENE_TIMES - 1)
    later = earlier + 1 + offset % (SCENE_TIMES - 1 - earlier)
    return jnp.stack([earlier, later]).astype(jnp.int32)


def plant(entries, rng, least, largest):
    extent = entries.shape
    index_at = [jax.random.randint(jax.random.fold_in(rng, axis), (), 0, extent[axis]) for axis in range(len(extent))]
    entries = entries.at[tuple(index_at)].set(least)
    longest = extent.index(max(extent))
    index_at[longest] = (index_at[longest] + 1) % extent[longest]
    return entries.at[tuple(index_at)].set(largest)


def level_of(key, extent, split, low, top_value):
    factor_of, own = 1.0, jax.random.fold_in(key, 6)
    for position, blocks in split:
        draws = jnp.exp(jax.random.uniform(jax.random.fold_in(own, position), (blocks,), jnp.float32, low / len(split), top_value / len(split)))
        factor_of = factor_of * jnp.repeat(draws, extent[position] // blocks).reshape([-1 if axis == position else 1 for axis in range(len(extent))])
    return factor_of


def noise(key, shape, width, most, split=(), kind=jnp.bfloat16):
    entries = jax.random.normal(key, shape, jnp.float32) * width
    if len(split) > 0:
        entries = level_of(key, shape, split, -0.22, 0.18) * entries
    return jnp.clip(entries, min=-most, max=most).astype(kind)


def setup_inputs(seed: int = 0) -> dict:
    arg_keys = jax.random.split(jax.random.key(seed), 7)
    prior_motion = noise(arg_keys[0], (REALIZATION_NUM, SCENE_TIMES, RASTER_CELLS), 1.0, 6.0, ((0, 8), (2, 4)))
    measured_motion = noise(arg_keys[1], (NOBS,), 0.2, 1.6, (), jnp.float32)
    measurement_noise_stddev = jnp.clip(jnp.exp(jax.random.uniform(arg_keys[2], (NOBS,), jnp.float32, math.log(0.05), math.log(0.5))), 0.05, 0.5)
    gaussian_jitter = noise(arg_keys[3], (PASS_COUNT, NOBS, REALIZATION_NUM), 1.0, 6.0, (), jnp.float32)
    scene_couples = draw_scene_couples(jax.random.fold_in(arg_keys[6], 71), 0)
    targeted_tile_number = plant(jax.random.randint(arg_keys[5], (NOBS,), 0, NBLK), jax.random.fold_in(arg_keys[5], 1), 0, NBLK - 1).astype(jnp.int32)
    return {"prior_motion": prior_motion, "measured_motion": measured_motion, "measurement_noise_stddev": measurement_noise_stddev, "gaussian_jitter": gaussian_jitter, "scene_couples": scene_couples, "targeted_tile_number": targeted_tile_number}


def update_tile(tile_state, mixing):
    realization_vectors = tile_state.shape[0]
    average = lax.optimization_barrier(jnp.sum(tile_state, axis=0, dtype=jnp.float32)) / realization_vectors
    anomaly = (tile_state.astype(jnp.float32) - average).astype(jnp.bfloat16)
    change = jnp.dot(mixing.T.astype(jnp.float32), anomaly.reshape(realization_vectors, -1).astype(jnp.float32), preferred_element_type=jnp.float32)
    return (tile_state.astype(jnp.float32) + change.reshape(tile_state.shape)).astype(jnp.bfloat16)

def reference(prior_motion, measured_motion, measurement_noise_stddev, gaussian_jitter, scene_couples, targeted_tile_number):
    realization_vectors = prior_motion.shape[0]
    spread_factor = float(PASS_COUNT)
    member_anomaly = jnp.sqrt(jnp.float32(spread_factor)) * measurement_noise_stddev
    ground_motion_vector = prior_motion
    for iteration in range(PASS_COUNT):
        sums = lax.optimization_barrier(jnp.sum(ground_motion_vector.reshape(realization_vectors, SCENE_TIMES, NBLK, BLK), axis=3, dtype=jnp.float32))
        predicted = ((sums[:, scene_couples[1], targeted_tile_number] - sums[:, scene_couples[0], targeted_tile_number]) / BLK).T
        centred = predicted - lax.optimization_barrier(jnp.mean(predicted, axis=1, keepdims=True))
        scaled = centred / (member_anomaly[:, None] * math.sqrt(realization_vectors - 1))
        misfit = (measured_motion[:, None] + member_anomaly[:, None] * gaussian_jitter[iteration] - predicted) / member_anomaly[:, None]
        gram = jnp.dot(scaled.T.astype(jnp.float32), scaled.astype(jnp.float32), precision=lax.Precision.HIGHEST, preferred_element_type=jnp.float32)
        cross = jnp.dot(scaled.T.astype(jnp.float32), misfit.astype(jnp.float32), precision=lax.Precision.HIGHEST, preferred_element_type=jnp.float32)
        factor = jnp.linalg.cholesky(jnp.eye(realization_vectors, dtype=jnp.float32) + gram)
        mixing = (jax.scipy.linalg.cho_solve((factor, True), cross) / math.sqrt(realization_vectors - 1)).astype(jnp.bfloat16)
        tiles = jnp.moveaxis(ground_motion_vector.reshape(realization_vectors, SCENE_TIMES, N_PIX * N_MEM, -1), 2, 0)

        def one_tile(tile_state):
            return update_tile(tile_state, mixing)
        fresh = lax.map(one_tile, tiles)
        ground_motion_vector = jnp.moveaxis(fresh, 0, 2).reshape(ground_motion_vector.shape)
    return ground_motion_vector
```

```python
import functools
import math

import jax
import jax.numpy as jnp
from jax import lax
from jax.experimental import pallas as pl
from jax.experimental.pallas import tpu as pltpu
from jax.sharding import PartitionSpec as P

BLK = 64
PASS_COUNT = 2
LANES = 128
CHUNKS = 4
F32 = jnp.float32
BF16 = jnp.bfloat16
HI = lax.Precision.HIGHEST
MESH = pl.DeviceIdType.MESH


def nn(a, b):
    return lax.dot_general(a, b, (((1,), (0,)), ((), ())), precision=HI, preferred_element_type=F32)


def tn(a, b):
    return nn(a.T, b)


def nt(a, b):
    return lax.dot_general(a, b, (((1,), (1,)), ((), ())), precision=HI, preferred_element_type=F32)


def iota(shape, axis):
    return lax.broadcasted_iota(jnp.int32, shape, axis)


def aligned(index, unit):
    return pl.ds(pl.multiple_of(index * unit, unit), unit)


def gauss_jordan(matrix, right, work):
    n = matrix.shape[0]
    work[...] = jnp.concatenate([matrix, right], axis=1)
    row_id = iota((n, 1), 0)
    lane_id = iota((n, 2 * n), 1)

    def step(k, carry):
        table = work[...]
        row = work[pl.ds(k, 1), :]
        here = lane_id == k
        factor = jnp.sum(jnp.where(here, table, 0.0), axis=1, keepdims=True)
        pivot = row / jnp.sum(jnp.where(here[:1], row, 0.0), axis=1, keepdims=True)
        work[...] = jnp.where(row_id == k, pivot, table - factor * pivot)
        return carry

    lax.fori_loop(0, n, step, 0)
    return work[:, n:]


def solve(total, work):
    n = total[0].shape[0]
    s, g = total[0][:, :n], total[0][:, n:]
    h1, h2 = total[1][:, :n], total[1][:, n:]
    eye = (iota((n, n), 0) == iota((n, n), 1)).astype(F32)
    m1 = gauss_jordan(eye + s / (n - 1), (g + h1 - s) / (n - 1), work).astype(BF16).astype(F32)
    m1_mean = jnp.mean(m1, axis=1, keepdims=True)
    step = eye + m1 - m1_mean
    s2 = tn(step, nn(s, step))
    g2 = tn(step, g - nn(s, jnp.broadcast_to(m1_mean, (n, n))))
    h22 = tn(step, h2)
    m2 = gauss_jordan(eye + s2 / (n - 1), (g2 + h22 - s2) / (n - 1), work).astype(BF16).astype(F32)
    m2c = m2 - jnp.mean(m2, axis=0, keepdims=True)
    w = m1 + m2 + nn(m1, m2c)
    return w - jnp.mean(w, axis=0, keepdims=True)


def expand(w, me, parts, times, mix):
    n = w.shape[0]
    members = n // parts
    rows = members * times
    depth = rows * parts
    spot = iota((n, n), 0)
    source = ((spot // members) ^ me) * members + spot % members
    order = (iota((n, n), 1) == source).astype(F32)
    wt = nt(nn(order, w.T), order)
    hi = wt.astype(BF16)
    lo = (wt - hi.astype(F32)).astype(BF16)
    spread = (iota((n, depth), 1) // times == iota((n, depth), 0)).astype(BF16)
    tall = (iota((rows, members), 0) // times == iota((rows, members), 1)).astype(BF16)
    same = iota((rows, depth), 0) % times == iota((rows, depth), 1) % times
    for piece, first in ((hi, 0), (lo, depth)):
        wide = jnp.dot(piece, spread, preferred_element_type=F32).astype(BF16)
        for part in range(parts):
            block = jnp.dot(
                tall, wide[part * members : (part + 1) * members, :], preferred_element_type=F32
            )
            start = first + part * rows
            mix[start : start + rows, :] = jnp.where(same, block, 0.0).astype(BF16)


def smoother_kernel(
    parts, tiles, times,
    prior, measured, noise, jitter, couples, target, out,
    state, fresh, mix, seen, summer, sums, work,
    measured_raw, noise_raw, couples_raw, target_raw, jitter_all,
    measured_row, noise_row, early_row, late_row, target_row,
    pred_out, pred_in, mine, members_in, stats_in,
    there_send, there_recv, back_send, back_recv,
    a_send, a_recv, b_send, b_recv, c_send, c_recv,
    look_sem, own_sem, small_sem,
):
    me = lax.axis_index("mem")
    tile = lax.axis_index("pix")
    rows, cells = prior.shape
    members = rows // times
    total_members = members * parts
    width = cells // parts
    span = width // CHUNKS
    obs = target.shape[1]
    padded = target_row.shape[1]
    share = padded // tiles
    tile_blocks = cells // BLK
    look = seen.shape[2]
    looks = cells // look

    def small(i, source, dest):
        return pltpu.make_async_copy(source, dest, small_sem.at[i])

    loads = [
        small(0, measured, measured_raw),
        small(1, noise, noise_raw),
        small(2, couples, couples_raw),
        small(3, target, target_raw),
        small(4, jitter, jitter_all.at[:, :obs, :]),
    ]

    def look_copy(i):
        return pltpu.make_async_copy(
            prior.at[:, aligned(i, look)], seen.at[lax.rem(i, 2)], look_sem.at[lax.rem(i, 2)]
        )

    own = pltpu.make_async_copy(prior.at[:, aligned(me, width)], state.at[pl.ds(0, rows), :], own_sem)

    def there(k, c):
        column = pl.multiple_of((me ^ k) * width + c * span, span)
        return pltpu.make_async_remote_copy(
            src_ref=prior.at[:, pl.ds(column, span)],
            dst_ref=state.at[pl.ds(k * rows, rows), pl.ds(c * span, span)],
            send_sem=there_send.at[k, c],
            recv_sem=there_recv.at[k, c],
            device_id={"mem": me ^ k},
            device_id_type=MESH,
        )

    def back(k, c):
        column = pl.multiple_of(me * width + c * span, span)
        return pltpu.make_async_remote_copy(
            src_ref=fresh.at[pl.ds(k * rows, rows), pl.ds(c * span, span)],
            dst_ref=out.at[:, pl.ds(column, span)],
            send_sem=back_send.at[k, c],
            recv_sem=back_recv.at[k, c],
            device_id={"mem": me ^ k},
            device_id_type=MESH,
        )

    def along(d):
        return lax.rem(tile + d, tiles)

    def send_a(d):
        return pltpu.make_async_remote_copy(
            src_ref=pred_out.at[along(d)],
            dst_ref=pred_in.at[tile],
            send_sem=a_send.at[d],
            recv_sem=a_recv.at[d],
            device_id={"pix": along(d)},
            device_id_type=MESH,
        )

    def send_b(k):
        return pltpu.make_async_remote_copy(
            src_ref=mine,
            dst_ref=members_in.at[me],
            send_sem=b_send.at[k],
            recv_sem=b_recv.at[k],
            device_id={"mem": me ^ k},
            device_id_type=MESH,
        )

    def send_c(d):
        return pltpu.make_async_remote_copy(
            src_ref=stats_in.at[tile],
            dst_ref=stats_in.at[tile],
            send_sem=c_send.at[d],
            recv_sem=c_recv.at[d],
            device_id={"pix": along(d)},
            device_id_type=MESH,
        )

    partners = list(reversed(range(1, parts)))
    others = list(range(1, tiles))

    barrier = pltpu.get_barrier_semaphore()
    for k in partners:
        pl.semaphore_signal(barrier, inc=1, device_id={"mem": me ^ k}, device_id_type=MESH)
    for d in others:
        pl.semaphore_signal(barrier, inc=1, device_id={"pix": along(d)}, device_id_type=MESH)
    look_copy(0).start()
    for load in loads:
        load.start()
    pl.semaphore_wait(barrier, len(partners) + len(others))
    for k in partners:
        there(k, 0).start()
    own.start()

    summer[...] = (iota((look, LANES), 0) // BLK == iota((look, LANES), 1)).astype(BF16)

    def look_step(i, carry):
        @pl.when(i + 1 < looks)
        def _():
            look_copy(i + 1).start()

        look_copy(i).wait()
        sums[:, aligned(i, LANES)] = jnp.dot(
            seen[lax.rem(i, 2)], summer[...], preferred_element_type=F32
        )
        return carry

    lax.fori_loop(0, looks, look_step, 0)

    for load in loads:
        load.wait()
    measured_row[...] = jnp.zeros((1, padded), F32)
    noise_row[...] = jnp.ones((1, padded), F32)
    early_row[...] = jnp.zeros((1, padded), jnp.int32)
    late_row[...] = jnp.zeros((1, padded), jnp.int32)
    target_row[...] = jnp.full((1, padded), -1, jnp.int32)
    measured_row[:, :obs] = measured_raw[...]
    noise_row[:, :obs] = noise_raw[...]
    early_row[:, :obs] = couples_raw[0:1, :]
    late_row[:, :obs] = couples_raw[1:2, :]
    target_row[:, :obs] = target_raw[...] - tile * tile_blocks
    jitter_all[:, obs:, :] = jnp.zeros((PASS_COUNT, padded - obs, total_members), F32)

    def predict(i, carry):
        lanes = aligned(i, share)
        table = (target_row[:, lanes] == iota((tile_blocks, share), 0)).astype(F32)
        part = nn(sums[...], table)
        scene = iota((rows, share), 0) % times
        pair = (scene == late_row[:, lanes]).astype(F32) - (scene == early_row[:, lanes]).astype(F32)
        group = (iota((members, rows), 1) // times == iota((members, rows), 0)).astype(F32)
        pred_out[i] = nn(group, part * pair) / BLK
        return carry

    lax.fori_loop(0, tiles, predict, 0)

    for d in others:
        send_a(d).start()
    pred_in[tile] = pred_out[tile]
    for d in others:
        send_a(d).wait()
    total = pred_in[0]
    for d in others:
        total = total + pred_in[d]
    mine[...] = total
    members_in[me] = total
    for k in partners:
        send_b(k).start()
    for c in range(1, CHUNKS):
        for k in partners:
            there(k, c).start()
    for k in partners:
        send_b(k).wait()

    pred = jnp.concatenate([members_in[i] for i in range(parts)], axis=0)
    lanes = aligned(tile, share)
    here = (iota((1, share), 1) + tile * share < obs).astype(F32)
    mean = jnp.mean(pred, axis=0, keepdims=True)
    scale = math.sqrt(float(PASS_COUNT)) * noise_row[:, lanes]
    centred = (pred - mean) / scale * here
    gap = jnp.broadcast_to((measured_row[:, lanes] - mean) / scale * here, pred.shape)
    shakes = jnp.concatenate([jitter_all[i, lanes, :] for i in range(PASS_COUNT)], axis=1)
    stats_in[tile, 0] = nt(centred, jnp.concatenate([centred, gap], axis=0))
    stats_in[tile, 1] = nn(centred, shakes)
    for d in others:
        send_c(d).start()
    for d in others:
        send_c(d).wait()
    total = stats_in[0]
    for d in others:
        total = total + stats_in[d]

    expand(solve(total, work), me, parts, times, mix)

    own.wait()
    step = math.gcd(span, 256)
    depth = parts * rows
    for c in range(CHUNKS):
        for k in partners:
            there(k, c).wait_recv()

        def update(i, carry):
            columns = pl.ds(pl.multiple_of(c * span + i * step, step), step)
            x = state[:, columns]
            both = jnp.dot(mix[...], x, preferred_element_type=F32)
            y = (x.astype(F32) + both[:depth] + both[depth:]).astype(BF16)
            fresh[:, columns] = y
            out[:, pl.ds(pl.multiple_of(me * width + c * span + i * step, step), step)] = y[:rows]
            return carry

        lax.fori_loop(0, span // step, update, 0)
        for k in partners:
            back(k, c).start()
    for c in range(CHUNKS):
        for k in partners:
            there(k, c).wait_send()
    for c in range(CHUNKS):
        for k in partners:
            back(k, c).wait()


def body(prior, measured, noise, jitter, couples, target):
    parts = lax.axis_size("mem")
    tiles = lax.axis_size("pix")
    members, times, cells = prior.shape
    total_members = members * parts
    rows = members * times
    depth = rows * parts
    width = cells // parts
    obs = target.shape[0]
    unit = LANES * tiles
    padded = obs + (-obs) % unit
    share = padded // tiles
    look = LANES * BLK
    anywhere = pl.BlockSpec(memory_space=pl.ANY)
    dma = pltpu.SemaphoreType.DMA
    scratch = [
        pltpu.VMEM((depth, width), BF16),
        pltpu.VMEM((depth, width), BF16),
        pltpu.VMEM((2 * depth, depth), BF16),
        pltpu.VMEM((2, rows, look), BF16),
        pltpu.VMEM((look, LANES), BF16),
        pltpu.VMEM((rows, cells // BLK), F32),
        pltpu.VMEM((total_members, 2 * total_members), F32),
        pltpu.VMEM((1, obs), F32),
        pltpu.VMEM((1, obs), F32),
        pltpu.VMEM((2, obs), jnp.int32),
        pltpu.VMEM((1, obs), jnp.int32),
        pltpu.VMEM((PASS_COUNT, padded, total_members), F32),
        pltpu.VMEM((1, padded), F32),
        pltpu.VMEM((1, padded), F32),
        pltpu.VMEM((1, padded), jnp.int32),
        pltpu.VMEM((1, padded), jnp.int32),
        pltpu.VMEM((1, padded), jnp.int32),
        pltpu.VMEM((tiles, members, share), F32),
        pltpu.VMEM((tiles, members, share), F32),
        pltpu.VMEM((members, share), F32),
        pltpu.VMEM((parts, members, share), F32),
        pltpu.VMEM((tiles, 2, total_members, 2 * total_members), F32),
        dma((parts, CHUNKS)),
        dma((parts, CHUNKS)),
        dma((parts, CHUNKS)),
        dma((parts, CHUNKS)),
        dma((tiles,)),
        dma((tiles,)),
        dma((parts,)),
        dma((parts,)),
        dma((tiles,)),
        dma((tiles,)),
        dma((2,)),
        dma,
        dma((5,)),
    ]
    out = pl.pallas_call(
        functools.partial(smoother_kernel, parts, tiles, times),
        in_specs=[anywhere] * 6,
        out_specs=pl.BlockSpec(memory_space=pltpu.VMEM),
        out_shape=jax.ShapeDtypeStruct((rows, cells), BF16),
        scratch_shapes=scratch,
        compiler_params=pltpu.CompilerParams(
            collective_id=0, has_side_effects=True, vmem_limit_bytes=52 * 1024 * 1024
        ),
        name="smoother",
    )(prior.reshape(rows, cells), measured[None, :], noise[None, :], jitter, couples, target[None, :])
    return out.reshape(prior.shape)


def solution(mesh):
    return jax.shard_map(
        body,
        mesh=mesh,
        in_specs=(P("mem", None, "pix"), P(), P(), P(), P(), P()),
        out_specs=P("mem", None, "pix"),
        check_vma=False,
    )
```

```python
import functools
import math

import jax
import jax.numpy as jnp
from jax import lax
from jax.experimental import pallas as pl
from jax.experimental.pallas import tpu as pltpu
from jax.sharding import PartitionSpec as P

BLK = 64
PASS_COUNT = 2
LANES = 128
CHUNKS = 4
F32 = jnp.float32
BF16 = jnp.bfloat16
HI = lax.Precision.HIGHEST
MESH = pl.DeviceIdType.MESH


def nn(a, b):
    return lax.dot_general(a, b, (((1,), (0,)), ((), ())), precision=HI, preferred_element_type=F32)


def tn(a, b):
    return nn(a.T, b)


def nt(a, b):
    return lax.dot_general(a, b, (((1,), (1,)), ((), ())), precision=HI, preferred_element_type=F32)


def iota(shape, axis):
    return lax.broadcasted_iota(jnp.int32, shape, axis)


def aligned(index, unit):
    return pl.ds(pl.multiple_of(index * unit, unit), unit)


def gauss_jordan(matrix, right, work):
    n = matrix.shape[0]
    work[...] = jnp.concatenate([matrix, right], axis=1)
    row_id = iota((n, 1), 0)
    lane_id = iota((n, 2 * n), 1)

    def step(k, carry):
        table = work[...]
        row = work[pl.ds(k, 1), :]
        here = lane_id == k
        factor = jnp.sum(jnp.where(here, table, 0.0), axis=1, keepdims=True)
        pivot = row / jnp.sum(jnp.where(here[:1], row, 0.0), axis=1, keepdims=True)
        work[...] = jnp.where(row_id == k, pivot, table - factor * pivot)
        return carry

    lax.fori_loop(0, n, step, 0)
    return work[:, n:]


def solve(total, work):
    n = total[0].shape[0]
    s, g = total[0][:, :n], total[0][:, n:]
    h1, h2 = total[1][:, :n], total[1][:, n:]
    eye = (iota((n, n), 0) == iota((n, n), 1)).astype(F32)
    m1 = gauss_jordan(eye + s / (n - 1), (g + h1 - s) / (n - 1), work).astype(BF16).astype(F32)
    m1_mean = jnp.mean(m1, axis=1, keepdims=True)
    step = eye + m1 - m1_mean
    s2 = tn(step, nn(s, step))
    g2 = tn(step, g - nn(s, jnp.broadcast_to(m1_mean, (n, n))))
    h22 = tn(step, h2)
    m2 = gauss_jordan(eye + s2 / (n - 1), (g2 + h22 - s2) / (n - 1), work).astype(BF16).astype(F32)
    m2c = m2 - jnp.mean(m2, axis=0, keepdims=True)
    w = m1 + m2 + nn(m1, m2c)
    return w - jnp.mean(w, axis=0, keepdims=True)


def expand(w, me, parts, times, mix):
    n = w.shape[0]
    members = n // parts
    rows = members * times
    depth = rows * parts
    spot = iota((n, n), 0)
    source = ((spot // members) ^ me) * members + spot % members
    order = (iota((n, n), 1) == source).astype(F32)
    wt = nt(nn(order, w.T), order)
    hi = wt.astype(BF16)
    lo = (wt - hi.astype(F32)).astype(BF16)
    spread = (iota((n, depth), 1) // times == iota((n, depth), 0)).astype(BF16)
    tall = (iota((rows, members), 0) // times == iota((rows, members), 1)).astype(BF16)
    same = iota((rows, depth), 0) % times == iota((rows, depth), 1) % times
    for piece, first in ((hi, 0), (lo, depth)):
        wide = jnp.dot(piece, spread, preferred_element_type=F32).astype(BF16)
        for part in range(parts):
            block = jnp.dot(
                tall, wide[part * members : (part + 1) * members, :], preferred_element_type=F32
            )
            start = first + part * rows
            mix[start : start + rows, :] = jnp.where(same, block, 0.0).astype(BF16)


def smoother_kernel(
    parts, tiles, times,
    prior, measured, noise, jitter, couples, target, out,
    state, mix, seen, summer, sums, work,
    measured_raw, noise_raw, couples_raw, target_raw, jitter_raw, jitter_all,
    measured_row, noise_row, early_row, late_row, target_row,
    pred_out, pred_in, mine, members_in, stats_in,
    there_send, there_recv, back_send, back_recv,
    a_send, a_recv, b_send, b_recv, c_send, c_recv,
    look_sem, own_sem, small_sem,
):
    me = lax.axis_index("mem")
    tile = lax.axis_index("pix")
    rows, cells = prior.shape
    members = rows // times
    total_members = members * parts
    width = cells // parts
    span = width // CHUNKS
    obs = target.shape[0]
    padded = target_row.shape[1]
    share = padded // tiles
    tile_blocks = cells // BLK
    look = seen.shape[2]
    looks = cells // look

    def small(i, source, dest):
        return pltpu.make_async_copy(source, dest, small_sem.at[i])

    loads = [
        small(0, measured, measured_raw),
        small(1, noise, noise_raw),
        small(2, couples, couples_raw),
        small(3, target, target_raw),
        small(4, jitter, jitter_raw),
    ]

    def look_copy(i):
        return pltpu.make_async_copy(
            prior.at[:, aligned(i, look)], seen.at[lax.rem(i, 2)], look_sem.at[lax.rem(i, 2)]
        )

    own = pltpu.make_async_copy(prior.at[:, aligned(me, width)], state.at[pl.ds(0, rows), :], own_sem)

    def there(k, c):
        column = pl.multiple_of((me ^ k) * width + c * span, span)
        return pltpu.make_async_remote_copy(
            src_ref=prior.at[:, pl.ds(column, span)],
            dst_ref=state.at[pl.ds(k * rows, rows), pl.ds(c * span, span)],
            send_sem=there_send.at[k, c],
            recv_sem=there_recv.at[k, c],
            device_id={"mem": me ^ k},
            device_id_type=MESH,
        )

    def back(k, c):
        column = pl.multiple_of(me * width + c * span, span)
        return pltpu.make_async_remote_copy(
            src_ref=state.at[pl.ds(k * rows, rows), pl.ds(c * span, span)],
            dst_ref=out.at[:, pl.ds(column, span)],
            send_sem=back_send.at[k, c],
            recv_sem=back_recv.at[k, c],
            device_id={"mem": me ^ k},
            device_id_type=MESH,
        )

    def along(d):
        return lax.rem(tile + d, tiles)

    def send_a(d):
        return pltpu.make_async_remote_copy(
            src_ref=pred_out.at[along(d)],
            dst_ref=pred_in.at[tile],
            send_sem=a_send.at[d],
            recv_sem=a_recv.at[d],
            device_id={"pix": along(d)},
            device_id_type=MESH,
        )

    def send_b(k):
        return pltpu.make_async_remote_copy(
            src_ref=mine,
            dst_ref=members_in.at[me],
            send_sem=b_send.at[k],
            recv_sem=b_recv.at[k],
            device_id={"mem": me ^ k},
            device_id_type=MESH,
        )

    def send_c(d):
        return pltpu.make_async_remote_copy(
            src_ref=stats_in.at[tile],
            dst_ref=stats_in.at[tile],
            send_sem=c_send.at[d],
            recv_sem=c_recv.at[d],
            device_id={"pix": along(d)},
            device_id_type=MESH,
        )

    partners = list(reversed(range(1, parts)))
    others = list(range(1, tiles))

    barrier = pltpu.get_barrier_semaphore()
    for k in partners:
        pl.semaphore_signal(barrier, inc=1, device_id={"mem": me ^ k}, device_id_type=MESH)
    for d in others:
        pl.semaphore_signal(barrier, inc=1, device_id={"pix": along(d)}, device_id_type=MESH)
    look_copy(0).start()
    for load in loads:
        load.start()
    pl.semaphore_wait(barrier, len(partners) + len(others))
    for k in partners:
        there(k, 0).start()
    own.start()

    summer[...] = (iota((look, LANES), 0) // BLK == iota((look, LANES), 1)).astype(BF16)

    def look_step(i, carry):
        @pl.when(i + 1 < looks)
        def _():
            look_copy(i + 1).start()

        look_copy(i).wait()
        sums[:, aligned(i, LANES)] = jnp.dot(
            seen[lax.rem(i, 2)], summer[...], preferred_element_type=F32
        )
        return carry

    lax.fori_loop(0, looks, look_step, 0)

    for load in loads:
        load.wait()
    measured_row[...] = jnp.zeros((1, padded), F32)
    noise_row[...] = jnp.ones((1, padded), F32)
    early_row[...] = jnp.zeros((1, padded), jnp.int32)
    late_row[...] = jnp.zeros((1, padded), jnp.int32)
    target_row[...] = jnp.full((1, padded), -1, jnp.int32)
    measured_row[:, :obs] = measured_raw[...].reshape(1, obs)
    noise_row[:, :obs] = noise_raw[...].reshape(1, obs)
    early_row[:, :obs] = couples_raw[0:1, :]
    late_row[:, :obs] = couples_raw[1:2, :]
    target_row[:, :obs] = target_raw[...].reshape(1, obs) - tile * tile_blocks
    jitter_all[...] = jnp.zeros((PASS_COUNT, total_members, padded), F32)
    jitter_all[:, :, :obs] = jitter_raw[...]

    def predict(i, carry):
        lanes = aligned(i, share)
        table = (target_row[:, lanes] == iota((tile_blocks, share), 0)).astype(F32)
        part = nn(sums[...], table)
        scene = iota((rows, share), 0) % times
        pair = (scene == late_row[:, lanes]).astype(F32) - (scene == early_row[:, lanes]).astype(F32)
        group = (iota((members, rows), 1) // times == iota((members, rows), 0)).astype(F32)
        pred_out[i] = nn(group, part * pair) / BLK
        return carry

    lax.fori_loop(0, tiles, predict, 0)

    for d in others:
        send_a(d).start()
    pred_in[tile] = pred_out[tile]
    for d in others:
        send_a(d).wait()
    total = pred_in[0]
    for d in others:
        total = total + pred_in[d]
    mine[...] = total
    members_in[me] = total
    for k in partners:
        send_b(k).start()
    for c in range(1, CHUNKS):
        for k in partners:
            there(k, c).start()
    for k in partners:
        send_b(k).wait()

    pred = jnp.concatenate([members_in[i] for i in range(parts)], axis=0)
    lanes = aligned(tile, share)
    here = (iota((1, share), 1) + tile * share < obs).astype(F32)
    mean = jnp.mean(pred, axis=0, keepdims=True)
    scale = math.sqrt(float(PASS_COUNT)) * noise_row[:, lanes]
    centred = (pred - mean) / scale * here
    gap = jnp.broadcast_to((measured_row[:, lanes] - mean) / scale * here, pred.shape)
    stats_in[tile, 0] = nt(centred, jnp.concatenate([centred, gap], axis=0))
    shakes = jnp.concatenate([jitter_all[i, :, lanes] for i in range(PASS_COUNT)], axis=0)
    stats_in[tile, 1] = nt(centred, shakes)
    for d in others:
        send_c(d).start()
    for d in others:
        send_c(d).wait()
    total = stats_in[0]
    for d in others:
        total = total + stats_in[d]

    expand(solve(total, work), me, parts, times, mix)

    own.wait()
    step = math.gcd(span, 256)
    depth = parts * rows
    for c in range(CHUNKS):
        for k in partners:
            there(k, c).wait_recv()

        def update(i, carry):
            columns = pl.ds(pl.multiple_of(c * span + i * step, step), step)
            x = state[:, columns]
            both = jnp.dot(mix[...], x, preferred_element_type=F32)
            y = (x.astype(F32) + both[:depth] + both[depth:]).astype(BF16)
            state[:, columns] = y
            out[:, pl.ds(pl.multiple_of(me * width + c * span + i * step, step), step)] = y[:rows]
            return carry

        lax.fori_loop(0, span // step, update, 0)
        for k in partners:
            back(k, c).start()
    for c in range(CHUNKS):
        for k in partners:
            there(k, c).wait_send()
    for c in range(CHUNKS):
        for k in partners:
            back(k, c).wait()


def body(prior, measured, noise, jitter, couples, target):
    parts = lax.axis_size("mem")
    tiles = lax.axis_size("pix")
    members, times, cells = prior.shape
    total_members = members * parts
    rows = members * times
    depth = rows * parts
    width = cells // parts
    obs = target.shape[0]
    unit = LANES * tiles
    padded = obs + (-obs) % unit
    share = padded // tiles
    look = LANES * BLK
    far = pl.BlockSpec(memory_space=pltpu.HBM)
    dma = pltpu.SemaphoreType.DMA
    scratch = [
        pltpu.VMEM((depth, width), BF16),
        pltpu.VMEM((2 * depth, depth), BF16),
        pltpu.VMEM((2, rows, look), BF16),
        pltpu.VMEM((look, LANES), BF16),
        pltpu.VMEM((rows, cells // BLK), F32),
        pltpu.VMEM((total_members, 2 * total_members), F32),
        pltpu.VMEM((obs,), F32),
        pltpu.VMEM((obs,), F32),
        pltpu.VMEM((2, obs), jnp.int32),
        pltpu.VMEM((obs,), jnp.int32),
        pltpu.VMEM((PASS_COUNT, total_members, obs), F32),
        pltpu.VMEM((PASS_COUNT, total_members, padded), F32),
        pltpu.VMEM((1, padded), F32),
        pltpu.VMEM((1, padded), F32),
        pltpu.VMEM((1, padded), jnp.int32),
        pltpu.VMEM((1, padded), jnp.int32),
        pltpu.VMEM((1, padded), jnp.int32),
        pltpu.VMEM((tiles, members, share), F32),
        pltpu.VMEM((tiles, members, share), F32),
        pltpu.VMEM((members, share), F32),
        pltpu.VMEM((parts, members, share), F32),
        pltpu.VMEM((tiles, 2, total_members, 2 * total_members), F32),
        dma((parts, CHUNKS)),
        dma((parts, CHUNKS)),
        dma((parts, CHUNKS)),
        dma((parts, CHUNKS)),
        dma((tiles,)),
        dma((tiles,)),
        dma((parts,)),
        dma((parts,)),
        dma((tiles,)),
        dma((tiles,)),
        dma((2,)),
        dma,
        dma((5,)),
    ]
    operands = (
        prior.reshape(rows, cells),
        measured,
        noise,
        jnp.swapaxes(jitter, 1, 2),
        couples,
        target,
    )
    out = pl.pallas_call(
        functools.partial(smoother_kernel, parts, tiles, times),
        in_specs=[far] * 6,
        out_specs=pl.BlockSpec(memory_space=pltpu.VMEM),
        out_shape=pltpu.VMEM((rows, cells), BF16),
        scratch_shapes=scratch,
        compiler_params=pltpu.CompilerParams(
            collective_id=0, has_side_effects=True, vmem_limit_bytes=44 * 1024 * 1024
        ),
        name="smoother",
    )(*(pltpu.with_memory_space_constraint(a, pltpu.HBM) for a in operands))
    return out.reshape(prior.shape)


def solution(mesh):
    return jax.shard_map(
        body,
        mesh=mesh,
        in_specs=(P("mem", None, "pix"), P(), P(), P(), P(), P()),
        out_specs=P("mem", None, "pix"),
        check_vma=False,
    )
```

```python
import functools
import math

import jax
import jax.numpy as jnp
from jax import lax
from jax.experimental import pallas as pl
from jax.experimental.pallas import tpu as pltpu
from jax.sharding import PartitionSpec as P

BLK = 64
PASS_COUNT = 2
LANES = 128
CHUNKS = 4
F32 = jnp.float32
BF16 = jnp.bfloat16
HI = lax.Precision.HIGHEST
MESH = pl.DeviceIdType.MESH


def nn(a, b):
    return lax.dot_general(a, b, (((1,), (0,)), ((), ())), precision=HI, preferred_element_type=F32)


def tn(a, b):
    return nn(a.T, b)


def nt(a, b):
    return lax.dot_general(a, b, (((1,), (1,)), ((), ())), precision=HI, preferred_element_type=F32)


def iota(shape, axis):
    return lax.broadcasted_iota(jnp.int32, shape, axis)


def aligned(index, unit):
    return pl.ds(pl.multiple_of(index * unit, unit), unit)


def gauss_jordan(matrix, right, work):
    n = matrix.shape[0]
    work[...] = jnp.concatenate([matrix, right], axis=1)
    row_id = iota((n, 1), 0)
    lane_id = iota((n, 2 * n), 1)

    def step(k, carry):
        table = work[...]
        row = work[pl.ds(k, 1), :]
        here = lane_id == k
        factor = jnp.sum(jnp.where(here, table, 0.0), axis=1, keepdims=True)
        pivot = row / jnp.sum(jnp.where(here[:1], row, 0.0), axis=1, keepdims=True)
        work[...] = jnp.where(row_id == k, pivot, table - factor * pivot)
        return carry

    lax.fori_loop(0, n, step, 0)
    return work[:, n:]


def solve(total, work):
    n = total[0].shape[0]
    s, g = total[0][:, :n], total[0][:, n:]
    h1, h2 = total[1][:, :n], total[1][:, n:]
    eye = (iota((n, n), 0) == iota((n, n), 1)).astype(F32)
    m1 = gauss_jordan(eye + s / (n - 1), (g + h1 - s) / (n - 1), work).astype(BF16).astype(F32)
    m1_mean = jnp.mean(m1, axis=1, keepdims=True)
    step = eye + m1 - m1_mean
    s2 = tn(step, nn(s, step))
    g2 = tn(step, g - nn(s, jnp.broadcast_to(m1_mean, (n, n))))
    h22 = tn(step, h2)
    m2 = gauss_jordan(eye + s2 / (n - 1), (g2 + h22 - s2) / (n - 1), work).astype(BF16).astype(F32)
    m2c = m2 - jnp.mean(m2, axis=0, keepdims=True)
    w = m1 + m2 + nn(m1, m2c)
    return w - jnp.mean(w, axis=0, keepdims=True)


def expand(w, me, parts, times, mix):
    n = w.shape[0]
    members = n // parts
    rows = members * times
    depth = rows * parts
    spot = iota((n, n), 0)
    source = ((spot // members) ^ me) * members + spot % members
    order = (iota((n, n), 1) == source).astype(F32)
    wt = nt(nn(order, w.T), order)
    hi = wt.astype(BF16)
    lo = (wt - hi.astype(F32)).astype(BF16)
    spread = (iota((n, depth), 1) // times == iota((n, depth), 0)).astype(BF16)
    tall = (iota((rows, members), 0) // times == iota((rows, members), 1)).astype(BF16)
    same = iota((rows, depth), 0) % times == iota((rows, depth), 1) % times
    for piece, first in ((hi, 0), (lo, depth)):
        wide = jnp.dot(piece, spread, preferred_element_type=F32).astype(BF16)
        for part in range(parts):
            block = jnp.dot(
                tall, wide[part * members : (part + 1) * members, :], preferred_element_type=F32
            )
            start = first + part * rows
            mix[start : start + rows, :] = jnp.where(same, block, 0.0).astype(BF16)


def smoother_kernel(
    parts, tiles, times,
    prior, measured, noise, jitter, couples, target, out,
    state, mix, seen, summer, sums, work,
    measured_raw, noise_raw, couples_raw, target_raw, jitter_raw, jitter_all,
    measured_row, noise_row, early_row, late_row, target_row,
    pred_out, pred_in, mine, members_in, stats_in,
    there_send, there_recv, back_send, back_recv,
    a_send, a_recv, b_send, b_recv, r_send, r_recv, c_send, c_recv,
    look_sem, own_sem, small_sem, go_sem,
):
    me = lax.axis_index("mem")
    tile = lax.axis_index("pix")
    rows, cells = prior.shape
    members = rows // times
    total_members = members * parts
    width = cells // parts
    span = width // CHUNKS
    obs = target.shape[0]
    padded = target_row.shape[1]
    share = padded // tiles
    tile_blocks = cells // BLK
    look = seen.shape[2]
    looks = cells // look

    def small(i, source, dest):
        return pltpu.make_async_copy(source, dest, small_sem.at[i])

    loads = [
        small(0, measured, measured_raw),
        small(1, noise, noise_raw),
        small(2, couples, couples_raw),
        small(3, target, target_raw),
        small(4, jitter, jitter_raw),
    ]

    def look_copy(i):
        return pltpu.make_async_copy(
            prior.at[:, aligned(i, look)], seen.at[lax.rem(i, 2)], look_sem.at[lax.rem(i, 2)]
        )

    own = pltpu.make_async_copy(prior.at[:, aligned(me, width)], state.at[pl.ds(0, rows), :], own_sem)

    def there(k, c):
        column = pl.multiple_of((me ^ k) * width + c * span, span)
        return pltpu.make_async_remote_copy(
            src_ref=prior.at[:, pl.ds(column, span)],
            dst_ref=state.at[pl.ds(k * rows, rows), pl.ds(c * span, span)],
            send_sem=there_send.at[k, c],
            recv_sem=there_recv.at[k, c],
            device_id={"mem": me ^ k},
            device_id_type=MESH,
        )

    def back(k, c):
        column = pl.multiple_of(me * width + c * span, span)
        return pltpu.make_async_remote_copy(
            src_ref=state.at[pl.ds(k * rows, rows), pl.ds(c * span, span)],
            dst_ref=out.at[:, pl.ds(column, span)],
            send_sem=back_send.at[k, c],
            recv_sem=back_recv.at[k, c],
            device_id={"mem": me ^ k},
            device_id_type=MESH,
        )

    def along(d):
        return lax.rem(tile + d, tiles)

    def send_a(d):
        return pltpu.make_async_remote_copy(
            src_ref=pred_out.at[along(d)],
            dst_ref=pred_in.at[tile],
            send_sem=a_send.at[d],
            recv_sem=a_recv.at[d],
            device_id={"pix": along(d)},
            device_id_type=MESH,
        )

    def send_b(k):
        return pltpu.make_async_remote_copy(
            src_ref=mine,
            dst_ref=members_in.at[me],
            send_sem=b_send.at[k],
            recv_sem=b_recv.at[k],
            device_id={"mem": me ^ k},
            device_id_type=MESH,
        )

    def relay(k):
        return pltpu.make_async_remote_copy(
            src_ref=members_in.at[me ^ k],
            dst_ref=members_in.at[me ^ k],
            send_sem=r_send.at[k],
            recv_sem=r_recv.at[k],
            device_id={"mem": me ^ 1},
            device_id_type=MESH,
        )

    def send_c(d):
        return pltpu.make_async_remote_copy(
            src_ref=stats_in.at[tile],
            dst_ref=stats_in.at[tile],
            send_sem=c_send.at[d],
            recv_sem=c_recv.at[d],
            device_id={"pix": along(d)},
            device_id_type=MESH,
        )

    partners = list(reversed(range(1, parts)))
    evens = partners[1::2]
    others = list(range(1, tiles))

    barrier = pltpu.get_barrier_semaphore()
    for k in partners:
        pl.semaphore_signal(barrier, inc=1, device_id={"mem": me ^ k}, device_id_type=MESH)
    look_copy(0).start()
    for load in loads:
        load.start()

    @pl.when(me != parts - 1)
    def _():
        pl.semaphore_wait(barrier, len(partners))

    @pl.when(me == parts - 2)
    def _():
        for d in others:
            there_id = {"mem": parts - 1, "pix": along(d)}
            pl.semaphore_signal(barrier, inc=1, device_id=there_id, device_id_type=MESH)

    @pl.when(me == parts - 1)
    def _():
        pl.semaphore_wait(barrier, len(partners) + len(others))
        for k in partners:
            pl.semaphore_signal(go_sem, inc=1, device_id={"mem": me ^ k}, device_id_type=MESH)

    for k in partners:
        there(k, 0).start()
    own.start()

    summer[...] = (iota((look, LANES), 0) // BLK == iota((look, LANES), 1)).astype(BF16)

    def look_step(i, carry):
        @pl.when(i + 1 < looks)
        def _():
            look_copy(i + 1).start()

        look_copy(i).wait()
        sums[:, aligned(i, LANES)] = jnp.dot(
            seen[lax.rem(i, 2)], summer[...], preferred_element_type=F32
        )
        return carry

    lax.fori_loop(0, looks, look_step, 0)

    for load in loads:
        load.wait()
    measured_row[...] = jnp.zeros((1, padded), F32)
    noise_row[...] = jnp.ones((1, padded), F32)
    early_row[...] = jnp.zeros((1, padded), jnp.int32)
    late_row[...] = jnp.zeros((1, padded), jnp.int32)
    target_row[...] = jnp.full((1, padded), -1, jnp.int32)
    measured_row[:, :obs] = measured_raw[...].reshape(1, obs)
    noise_row[:, :obs] = noise_raw[...].reshape(1, obs)
    early_row[:, :obs] = couples_raw[0:1, :]
    late_row[:, :obs] = couples_raw[1:2, :]
    target_row[:, :obs] = target_raw[...].reshape(1, obs) - tile * tile_blocks
    jitter_all[...] = jnp.zeros((PASS_COUNT, total_members, padded), F32)
    jitter_all[:, :, :obs] = jitter_raw[...]

    def predict(i, carry):
        lanes = aligned(i, share)
        table = (target_row[:, lanes] == iota((tile_blocks, share), 0)).astype(F32)
        part = nn(sums[...], table)
        scene = iota((rows, share), 0) % times
        pair = (scene == late_row[:, lanes]).astype(F32) - (scene == early_row[:, lanes]).astype(F32)
        group = (iota((members, rows), 1) // times == iota((members, rows), 0)).astype(F32)
        pred_out[i] = nn(group, part * pair) / BLK
        return carry

    lax.fori_loop(0, tiles, predict, 0)

    @pl.when(me != parts - 1)
    def _():
        pl.semaphore_wait(go_sem, 1)

    for d in others:
        send_a(d).start()
    pred_in[tile] = pred_out[tile]
    for d in others:
        send_a(d).wait()
    total = pred_in[0]
    for d in others:
        total = total + pred_in[d]
    mine[...] = total
    members_in[me] = total
    for k in evens + [1]:
        send_b(k).start()
    for c in range(1, CHUNKS):
        for k in partners:
            there(k, c).start()
    for k in evens:
        send_b(k).wait()
        relay(k).start()
    send_b(1).wait()
    for k in evens:
        relay(k).wait()

    pred = jnp.concatenate([members_in[i] for i in range(parts)], axis=0)
    lanes = aligned(tile, share)
    here = (iota((1, share), 1) + tile * share < obs).astype(F32)
    mean = jnp.mean(pred, axis=0, keepdims=True)
    scale = math.sqrt(float(PASS_COUNT)) * noise_row[:, lanes]
    centred = (pred - mean) / scale * here
    gap = jnp.broadcast_to((measured_row[:, lanes] - mean) / scale * here, pred.shape)
    stats_in[tile, 0] = nt(centred, jnp.concatenate([centred, gap], axis=0))
    shakes = jnp.concatenate([jitter_all[i, :, lanes] for i in range(PASS_COUNT)], axis=0)
    stats_in[tile, 1] = nt(centred, shakes)
    for d in others:
        send_c(d).start()
    for d in others:
        send_c(d).wait()
    total = stats_in[0]
    for d in others:
        total = total + stats_in[d]

    expand(solve(total, work), me, parts, times, mix)

    own.wait()
    step = math.gcd(span, 256)
    depth = parts * rows
    for c in range(CHUNKS):
        for k in partners:
            there(k, c).wait_recv()

        def update(i, carry):
            columns = pl.ds(pl.multiple_of(c * span + i * step, step), step)
            x = state[:, columns]
            both = jnp.dot(mix[...], x, preferred_element_type=F32)
            y = (x.astype(F32) + both[:depth] + both[depth:]).astype(BF16)
            state[:, columns] = y
            out[:, pl.ds(pl.multiple_of(me * width + c * span + i * step, step), step)] = y[:rows]
            return carry

        lax.fori_loop(0, span // step, update, 0)
        for k in partners:
            back(k, c).start()
    for c in range(CHUNKS):
        for k in partners:
            there(k, c).wait_send()
    for c in range(CHUNKS):
        for k in partners:
            back(k, c).wait()


def body(prior, measured, noise, jitter, couples, target):
    parts = lax.axis_size("mem")
    tiles = lax.axis_size("pix")
    members, times, cells = prior.shape
    total_members = members * parts
    rows = members * times
    depth = rows * parts
    width = cells // parts
    obs = target.shape[0]
    unit = LANES * tiles
    padded = obs + (-obs) % unit
    share = padded // tiles
    look = LANES * BLK
    far = pl.BlockSpec(memory_space=pltpu.HBM)
    dma = pltpu.SemaphoreType.DMA
    scratch = [
        pltpu.VMEM((depth, width), BF16),
        pltpu.VMEM((2 * depth, depth), BF16),
        pltpu.VMEM((2, rows, look), BF16),
        pltpu.VMEM((look, LANES), BF16),
        pltpu.VMEM((rows, cells // BLK), F32),
        pltpu.VMEM((total_members, 2 * total_members), F32),
        pltpu.VMEM((obs,), F32),
        pltpu.VMEM((obs,), F32),
        pltpu.VMEM((2, obs), jnp.int32),
        pltpu.VMEM((obs,), jnp.int32),
        pltpu.VMEM((PASS_COUNT, total_members, obs), F32),
        pltpu.VMEM((PASS_COUNT, total_members, padded), F32),
        pltpu.VMEM((1, padded), F32),
        pltpu.VMEM((1, padded), F32),
        pltpu.VMEM((1, padded), jnp.int32),
        pltpu.VMEM((1, padded), jnp.int32),
        pltpu.VMEM((1, padded), jnp.int32),
        pltpu.VMEM((tiles, members, share), F32),
        pltpu.VMEM((tiles, members, share), F32),
        pltpu.VMEM((members, share), F32),
        pltpu.VMEM((parts, members, share), F32),
        pltpu.VMEM((tiles, 2, total_members, 2 * total_members), F32),
        dma((parts, CHUNKS)),
        dma((parts, CHUNKS)),
        dma((parts, CHUNKS)),
        dma((parts, CHUNKS)),
        dma((tiles,)),
        dma((tiles,)),
        dma((parts,)),
        dma((parts,)),
        dma((parts,)),
        dma((parts,)),
        dma((tiles,)),
        dma((tiles,)),
        dma((2,)),
        dma,
        dma((5,)),
        pltpu.SemaphoreType.REGULAR,
    ]
    operands = (
        prior.reshape(rows, cells),
        measured,
        noise,
        jnp.swapaxes(jitter, 1, 2),
        couples,
        target,
    )
    out = pl.pallas_call(
        functools.partial(smoother_kernel, parts, tiles, times),
        in_specs=[far] * 6,
        out_specs=pl.BlockSpec(memory_space=pltpu.VMEM),
        out_shape=pltpu.VMEM((rows, cells), BF16),
        scratch_shapes=scratch,
        compiler_params=pltpu.CompilerParams(
            collective_id=0, has_side_effects=True, vmem_limit_bytes=44 * 1024 * 1024
        ),
        name="smoother",
    )(*(pltpu.with_memory_space_constraint(a, pltpu.HBM) for a in operands))
    return out.reshape(prior.shape)


def solution(mesh):
    return jax.shard_map(
        body,
        mesh=mesh,
        in_specs=(P("mem", None, "pix"), P(), P(), P(), P(), P()),
        out_specs=P("mem", None, "pix"),
        check_vma=False,
    )
```

```python
import functools
import math

import jax
import jax.numpy as jnp
from jax import lax
from jax.experimental import pallas as pl
from jax.experimental.pallas import tpu as pltpu
from jax.sharding import PartitionSpec as P

BLK = 64
PASS_COUNT = 2
LANES = 128
CHUNKS = 4
F32 = jnp.float32
BF16 = jnp.bfloat16
HI = lax.Precision.HIGHEST
MESH = pl.DeviceIdType.MESH


def nn(a, b):
    return lax.dot_general(a, b, (((1,), (0,)), ((), ())), precision=HI, preferred_element_type=F32)


def tn(a, b):
    return nn(a.T, b)


def nt(a, b):
    return lax.dot_general(a, b, (((1,), (1,)), ((), ())), precision=HI, preferred_element_type=F32)


def iota(shape, axis):
    return lax.broadcasted_iota(jnp.int32, shape, axis)


def aligned(index, unit):
    return pl.ds(pl.multiple_of(index * unit, unit), unit)


def gauss_jordan(matrix, right, work):
    n = matrix.shape[0]
    work[...] = jnp.concatenate([matrix, right], axis=1)
    row_id = iota((n, 1), 0)
    lane_id = iota((n, 2 * n), 1)

    def step(k, carry):
        table = work[...]
        row = work[pl.ds(k, 1), :]
        here = lane_id == k
        factor = jnp.sum(jnp.where(here, table, 0.0), axis=1, keepdims=True)
        pivot = row / jnp.sum(jnp.where(here[:1], row, 0.0), axis=1, keepdims=True)
        work[...] = jnp.where(row_id == k, pivot, table - factor * pivot)
        return carry

    lax.fori_loop(0, n, step, 0)
    return work[:, n:]


def solve(total, work):
    n = total[0].shape[0]
    s, g = total[0][:, :n], total[0][:, n:]
    h1, h2 = total[1][:, :n], total[1][:, n:]
    eye = (iota((n, n), 0) == iota((n, n), 1)).astype(F32)
    m1 = gauss_jordan(eye + s / (n - 1), (g + h1 - s) / (n - 1), work).astype(BF16).astype(F32)
    m1_mean = jnp.mean(m1, axis=1, keepdims=True)
    step = eye + m1 - m1_mean
    s2 = tn(step, nn(s, step))
    g2 = tn(step, g - nn(s, jnp.broadcast_to(m1_mean, (n, n))))
    h22 = tn(step, h2)
    m2 = gauss_jordan(eye + s2 / (n - 1), (g2 + h22 - s2) / (n - 1), work).astype(BF16).astype(F32)
    m2c = m2 - jnp.mean(m2, axis=0, keepdims=True)
    w = m1 + m2 + nn(m1, m2c)
    return w - jnp.mean(w, axis=0, keepdims=True)


def expand(w, me, parts, times, mix):
    n = w.shape[0]
    members = n // parts
    rows = members * times
    depth = rows * parts
    spot = iota((n, n), 0)
    source = ((spot // members) ^ me) * members + spot % members
    order = (iota((n, n), 1) == source).astype(F32)
    wt = nt(nn(order, w.T), order)
    hi = wt.astype(BF16)
    lo = (wt - hi.astype(F32)).astype(BF16)
    spread = (iota((n, depth), 1) // times == iota((n, depth), 0)).astype(BF16)
    tall = (iota((rows, members), 0) // times == iota((rows, members), 1)).astype(BF16)
    same = iota((rows, depth), 0) % times == iota((rows, depth), 1) % times
    for piece, first in ((hi, 0), (lo, depth)):
        wide = jnp.dot(piece, spread, preferred_element_type=F32).astype(BF16)
        for part in range(parts):
            block = jnp.dot(
                tall, wide[part * members : (part + 1) * members, :], preferred_element_type=F32
            )
            start = first + part * rows
            mix[start : start + rows, :] = jnp.where(same, block, 0.0).astype(BF16)


def smoother_kernel(
    parts, tiles, times,
    prior, measured, noise, jitter, couples, target, out,
    state, mix, seen, summer, sums, work,
    measured_raw, noise_raw, couples_raw, target_raw, jitter_raw, jitter_all,
    measured_row, noise_row, early_row, late_row, target_row,
    pred_out, pred_in, mine, members_in, stats_in,
    there_send, there_recv, back_send, back_recv,
    a_send, a_recv, b_send, b_recv, r_send, r_recv, c_send, c_recv,
    look_sem, own_sem, small_sem, go_sem,
):
    me = lax.axis_index("mem")
    tile = lax.axis_index("pix")
    rows, cells = prior.shape
    members = rows // times
    total_members = members * parts
    width = cells // parts
    span = width // CHUNKS
    obs = target.shape[0]
    padded = target_row.shape[1]
    share = padded // tiles
    tile_blocks = cells // BLK
    look = seen.shape[2]
    looks = cells // look

    def small(i, source, dest):
        return pltpu.make_async_copy(source, dest, small_sem.at[i])

    loads = [
        small(0, measured, measured_raw),
        small(1, noise, noise_raw),
        small(2, couples, couples_raw),
        small(3, target, target_raw),
        small(4, jitter, jitter_raw),
    ]

    def look_copy(i):
        return pltpu.make_async_copy(
            prior.at[:, aligned(i, look)], seen.at[lax.rem(i, 2)], look_sem.at[lax.rem(i, 2)]
        )

    own = pltpu.make_async_copy(prior.at[:, aligned(me, width)], state.at[pl.ds(0, rows), :], own_sem)

    def there(k, c):
        column = pl.multiple_of((me ^ k) * width + c * span, span)
        return pltpu.make_async_remote_copy(
            src_ref=prior.at[:, pl.ds(column, span)],
            dst_ref=state.at[pl.ds(k * rows, rows), pl.ds(c * span, span)],
            send_sem=there_send.at[k, c],
            recv_sem=there_recv.at[k, c],
            device_id={"mem": me ^ k},
            device_id_type=MESH,
        )

    def back(k, c):
        column = pl.multiple_of(me * width + c * span, span)
        return pltpu.make_async_remote_copy(
            src_ref=state.at[pl.ds(k * rows, rows), pl.ds(c * span, span)],
            dst_ref=out.at[:, pl.ds(column, span)],
            send_sem=back_send.at[k, c],
            recv_sem=back_recv.at[k, c],
            device_id={"mem": me ^ k},
            device_id_type=MESH,
        )

    def along(d):
        return lax.rem(tile + d, tiles)

    def send_a(d):
        return pltpu.make_async_remote_copy(
            src_ref=pred_out.at[along(d)],
            dst_ref=pred_in.at[tile],
            send_sem=a_send.at[d],
            recv_sem=a_recv.at[d],
            device_id={"pix": along(d)},
            device_id_type=MESH,
        )

    def send_b(k):
        return pltpu.make_async_remote_copy(
            src_ref=mine,
            dst_ref=members_in.at[me],
            send_sem=b_send.at[k],
            recv_sem=b_recv.at[k],
            device_id={"mem": me ^ k},
            device_id_type=MESH,
        )

    def relay(k):
        return pltpu.make_async_remote_copy(
            src_ref=members_in.at[me ^ k],
            dst_ref=members_in.at[me ^ k],
            send_sem=r_send.at[k],
            recv_sem=r_recv.at[k],
            device_id={"mem": me ^ 1},
            device_id_type=MESH,
        )

    def send_c(d):
        return pltpu.make_async_remote_copy(
            src_ref=stats_in.at[tile],
            dst_ref=stats_in.at[tile],
            send_sem=c_send.at[d],
            recv_sem=c_recv.at[d],
            device_id={"pix": along(d)},
            device_id_type=MESH,
        )

    partners = list(reversed(range(1, parts)))
    evens = partners[1::2]
    others = list(range(1, tiles))

    barrier = pltpu.get_barrier_semaphore()
    for k in partners:
        pl.semaphore_signal(barrier, inc=1, device_id={"mem": me ^ k}, device_id_type=MESH)
    look_copy(0).start()
    for load in loads:
        load.start()

    speaker = me == parts - 1
    root = jnp.logical_and(speaker, tile == tiles - 1)
    branch = jnp.logical_and(speaker, tile != tiles - 1)

    @pl.when(jnp.logical_not(root))
    def _():
        pl.semaphore_wait(barrier, len(partners))

    @pl.when(branch)
    def _():
        root_id = {"mem": me, "pix": tiles - 1}
        pl.semaphore_signal(barrier, inc=1, device_id=root_id, device_id_type=MESH)

    @pl.when(root)
    def _():
        pl.semaphore_wait(barrier, len(partners) + len(others))
        for d in others:
            pl.semaphore_signal(go_sem, inc=1, device_id={"pix": along(d)}, device_id_type=MESH)
        for k in partners:
            pl.semaphore_signal(go_sem, inc=1, device_id={"mem": me ^ k}, device_id_type=MESH)

    for k in partners:
        there(k, 0).start()
    own.start()

    summer[...] = (iota((look, LANES), 0) // BLK == iota((look, LANES), 1)).astype(BF16)

    def look_step(i, carry):
        @pl.when(i + 1 < looks)
        def _():
            look_copy(i + 1).start()

        look_copy(i).wait()
        sums[:, aligned(i, LANES)] = jnp.dot(
            seen[lax.rem(i, 2)], summer[...], preferred_element_type=F32
        )
        return carry

    lax.fori_loop(0, looks, look_step, 0)

    for load in loads:
        load.wait()
    measured_row[...] = jnp.zeros((1, padded), F32)
    noise_row[...] = jnp.ones((1, padded), F32)
    early_row[...] = jnp.zeros((1, padded), jnp.int32)
    late_row[...] = jnp.zeros((1, padded), jnp.int32)
    target_row[...] = jnp.full((1, padded), -1, jnp.int32)
    measured_row[:, :obs] = measured_raw[...].reshape(1, obs)
    noise_row[:, :obs] = noise_raw[...].reshape(1, obs)
    early_row[:, :obs] = couples_raw[0:1, :]
    late_row[:, :obs] = couples_raw[1:2, :]
    target_row[:, :obs] = target_raw[...].reshape(1, obs) - tile * tile_blocks
    jitter_all[...] = jnp.zeros((PASS_COUNT, total_members, padded), F32)
    jitter_all[:, :, :obs] = jitter_raw[...]

    def predict(i, carry):
        lanes = aligned(i, share)
        table = (target_row[:, lanes] == iota((tile_blocks, share), 0)).astype(F32)
        part = nn(sums[...], table)
        scene = iota((rows, share), 0) % times
        pair = (scene == late_row[:, lanes]).astype(F32) - (scene == early_row[:, lanes]).astype(F32)
        group = (iota((members, rows), 1) // times == iota((members, rows), 0)).astype(F32)
        pred_out[i] = nn(group, part * pair) / BLK
        return carry

    lax.fori_loop(0, tiles, predict, 0)

    @pl.when(jnp.logical_not(root))
    def _():
        pl.semaphore_wait(go_sem, 1)

    @pl.when(branch)
    def _():
        for k in partners:
            pl.semaphore_signal(go_sem, inc=1, device_id={"mem": me ^ k}, device_id_type=MESH)

    for d in others:
        send_a(d).start()
    pred_in[tile] = pred_out[tile]
    for d in others:
        send_a(d).wait()
    total = pred_in[0]
    for d in others:
        total = total + pred_in[d]
    mine[...] = total
    members_in[me] = total
    for k in evens + [1]:
        send_b(k).start()
    for c in range(1, CHUNKS):
        for k in partners:
            there(k, c).start()
    for k in evens:
        send_b(k).wait()
        relay(k).start()
    send_b(1).wait()
    for k in evens:
        relay(k).wait()

    pred = jnp.concatenate([members_in[i] for i in range(parts)], axis=0)
    lanes = aligned(tile, share)
    here = (iota((1, share), 1) + tile * share < obs).astype(F32)
    mean = jnp.mean(pred, axis=0, keepdims=True)
    scale = math.sqrt(float(PASS_COUNT)) * noise_row[:, lanes]
    centred = (pred - mean) / scale * here
    gap = jnp.broadcast_to((measured_row[:, lanes] - mean) / scale * here, pred.shape)
    stats_in[tile, 0] = nt(centred, jnp.concatenate([centred, gap], axis=0))
    shakes = jnp.concatenate([jitter_all[i, :, lanes] for i in range(PASS_COUNT)], axis=0)
    stats_in[tile, 1] = nt(centred, shakes)
    for d in others:
        send_c(d).start()
    for d in others:
        send_c(d).wait()
    total = stats_in[0]
    for d in others:
        total = total + stats_in[d]

    expand(solve(total, work), me, parts, times, mix)

    own.wait()
    step = math.gcd(span, 256)
    depth = parts * rows
    for c in range(CHUNKS):
        for k in partners:
            there(k, c).wait_recv()

        def update(i, carry):
            columns = pl.ds(pl.multiple_of(c * span + i * step, step), step)
            x = state[:, columns]
            both = jnp.dot(mix[...], x, preferred_element_type=F32)
            y = (x.astype(F32) + both[:depth] + both[depth:]).astype(BF16)
            state[:, columns] = y
            out[:, pl.ds(pl.multiple_of(me * width + c * span + i * step, step), step)] = y[:rows]
            return carry

        lax.fori_loop(0, span // step, update, 0)
        for k in partners:
            back(k, c).start()
    for c in range(CHUNKS):
        for k in partners:
            there(k, c).wait_send()
    for c in range(CHUNKS):
        for k in partners:
            back(k, c).wait()


def body(prior, measured, noise, jitter, couples, target):
    parts = lax.axis_size("mem")
    tiles = lax.axis_size("pix")
    members, times, cells = prior.shape
    total_members = members * parts
    rows = members * times
    depth = rows * parts
    width = cells // parts
    obs = target.shape[0]
    unit = LANES * tiles
    padded = obs + (-obs) % unit
    share = padded // tiles
    look = LANES * BLK
    far = pl.BlockSpec(memory_space=pltpu.HBM)
    dma = pltpu.SemaphoreType.DMA
    scratch = [
        pltpu.VMEM((depth, width), BF16),
        pltpu.VMEM((2 * depth, depth), BF16),
        pltpu.VMEM((2, rows, look), BF16),
        pltpu.VMEM((look, LANES), BF16),
        pltpu.VMEM((rows, cells // BLK), F32),
        pltpu.VMEM((total_members, 2 * total_members), F32),
        pltpu.VMEM((obs,), F32),
        pltpu.VMEM((obs,), F32),
        pltpu.VMEM((2, obs), jnp.int32),
        pltpu.VMEM((obs,), jnp.int32),
        pltpu.VMEM((PASS_COUNT, total_members, obs), F32),
        pltpu.VMEM((PASS_COUNT, total_members, padded), F32),
        pltpu.VMEM((1, padded), F32),
        pltpu.VMEM((1, padded), F32),
        pltpu.VMEM((1, padded), jnp.int32),
        pltpu.VMEM((1, padded), jnp.int32),
        pltpu.VMEM((1, padded), jnp.int32),
        pltpu.VMEM((tiles, members, share), F32),
        pltpu.VMEM((tiles, members, share), F32),
        pltpu.VMEM((members, share), F32),
        pltpu.VMEM((parts, members, share), F32),
        pltpu.VMEM((tiles, 2, total_members, 2 * total_members), F32),
        dma((parts, CHUNKS)),
        dma((parts, CHUNKS)),
        dma((parts, CHUNKS)),
        dma((parts, CHUNKS)),
        dma((tiles,)),
        dma((tiles,)),
        dma((parts,)),
        dma((parts,)),
        dma((parts,)),
        dma((parts,)),
        dma((tiles,)),
        dma((tiles,)),
        dma((2,)),
        dma,
        dma((5,)),
        pltpu.SemaphoreType.REGULAR,
    ]
    operands = (
        prior.reshape(rows, cells),
        measured,
        noise,
        jnp.swapaxes(jitter, 1, 2),
        couples,
        target,
    )
    out = pl.pallas_call(
        functools.partial(smoother_kernel, parts, tiles, times),
        in_specs=[far] * 6,
        out_specs=pl.BlockSpec(memory_space=pltpu.VMEM),
        out_shape=pltpu.VMEM((rows, cells), BF16),
        scratch_shapes=scratch,
        compiler_params=pltpu.CompilerParams(
            collective_id=0, has_side_effects=True, vmem_limit_bytes=44 * 1024 * 1024
        ),
        name="smoother",
    )(*(pltpu.with_memory_space_constraint(a, pltpu.HBM) for a in operands))
    return out.reshape(prior.shape)


def solution(mesh):
    return jax.shard_map(
        body,
        mesh=mesh,
        in_specs=(P("mem", None, "pix"), P(), P(), P(), P(), P()),
        out_specs=P("mem", None, "pix"),
        check_vma=False,
    )
```

```python
import functools
import math

import jax
import jax.numpy as jnp
from jax import lax
from jax.experimental import pallas as pl
from jax.experimental.pallas import tpu as pltpu
from jax.sharding import PartitionSpec as P

BLK = 64
PASS_COUNT = 2
LANES = 128
CHUNKS = 4
F32 = jnp.float32
BF16 = jnp.bfloat16
HI = lax.Precision.HIGHEST
MESH = pl.DeviceIdType.MESH


def nn(a, b):
    return lax.dot_general(a, b, (((1,), (0,)), ((), ())), precision=HI, preferred_element_type=F32)


def tn(a, b):
    return nn(a.T, b)


def nt(a, b):
    return lax.dot_general(a, b, (((1,), (1,)), ((), ())), precision=HI, preferred_element_type=F32)


def iota(shape, axis):
    return lax.broadcasted_iota(jnp.int32, shape, axis)


def aligned(index, unit):
    return pl.ds(pl.multiple_of(index * unit, unit), unit)


def gauss_jordan(matrix, right, work):
    n = matrix.shape[0]
    work[...] = jnp.concatenate([matrix, right], axis=1)
    row_id = iota((n, 1), 0)
    lane_id = iota((n, 2 * n), 1)

    def step(k, carry):
        table = work[...]
        row = work[pl.ds(k, 1), :]
        here = lane_id == k
        factor = jnp.sum(jnp.where(here, table, 0.0), axis=1, keepdims=True)
        pivot = row / jnp.sum(jnp.where(here[:1], row, 0.0), axis=1, keepdims=True)
        work[...] = jnp.where(row_id == k, pivot, table - factor * pivot)
        return carry

    lax.fori_loop(0, n, step, 0)
    return work[:, n:]


def solve(total, work):
    n = total[0].shape[0]
    s, g = total[0][:, :n], total[0][:, n:]
    h1, h2 = total[1][:, :n], total[1][:, n:]
    eye = (iota((n, n), 0) == iota((n, n), 1)).astype(F32)
    m1 = gauss_jordan(eye + s / (n - 1), (g + h1 - s) / (n - 1), work).astype(BF16).astype(F32)
    m1_mean = jnp.mean(m1, axis=1, keepdims=True)
    step = eye + m1 - m1_mean
    s2 = tn(step, nn(s, step))
    g2 = tn(step, g - nn(s, jnp.broadcast_to(m1_mean, (n, n))))
    h22 = tn(step, h2)
    m2 = gauss_jordan(eye + s2 / (n - 1), (g2 + h22 - s2) / (n - 1), work).astype(BF16).astype(F32)
    m2c = m2 - jnp.mean(m2, axis=0, keepdims=True)
    w = m1 + m2 + nn(m1, m2c)
    return w - jnp.mean(w, axis=0, keepdims=True)


def expand(w, me, parts, times, mix):
    n = w.shape[0]
    members = n // parts
    rows = members * times
    depth = rows * parts
    spot = iota((n, n), 0)
    source = ((spot // members) ^ me) * members + spot % members
    order = (iota((n, n), 1) == source).astype(F32)
    wt = nt(nn(order, w.T), order)
    hi = wt.astype(BF16)
    lo = (wt - hi.astype(F32)).astype(BF16)
    spread = (iota((n, depth), 1) // times == iota((n, depth), 0)).astype(BF16)
    tall = (iota((rows, members), 0) // times == iota((rows, members), 1)).astype(BF16)
    same = iota((rows, depth), 0) % times == iota((rows, depth), 1) % times
    for piece, first in ((hi, 0), (lo, depth)):
        wide = jnp.dot(piece, spread, preferred_element_type=F32).astype(BF16)
        for part in range(parts):
            block = jnp.dot(
                tall, wide[part * members : (part + 1) * members, :], preferred_element_type=F32
            )
            start = first + part * rows
            mix[start : start + rows, :] = jnp.where(same, block, 0.0).astype(BF16)


def smoother_kernel(
    parts, tiles, times,
    prior, measured, noise, jitter, couples, target, out,
    state, mix, seen, summer, sums, work,
    measured_raw, noise_raw, couples_raw, target_raw, jitter_raw, jitter_all,
    measured_row, noise_row, early_row, late_row, target_row,
    pred_out, pred_in, mine, members_in, stats_in,
    there_send, there_recv, back_send, back_recv,
    a_send, a_recv, b_send, b_recv, r_send, r_recv, c_send, c_recv,
    look_sem, own_sem, small_sem, go_sem,
):
    me = lax.axis_index("mem")
    tile = lax.axis_index("pix")
    rows, cells = prior.shape
    members = rows // times
    total_members = members * parts
    width = cells // parts
    span = width // CHUNKS
    obs = target.shape[0]
    padded = target_row.shape[1]
    share = padded // tiles
    tile_blocks = cells // BLK
    look = seen.shape[2]
    looks = cells // look

    def small(i, source, dest):
        return pltpu.make_async_copy(source, dest, small_sem.at[i])

    loads = [
        small(0, measured, measured_raw),
        small(1, noise, noise_raw),
        small(2, couples, couples_raw),
        small(3, target, target_raw),
        small(4, jitter, jitter_raw),
    ]

    def look_copy(i):
        return pltpu.make_async_copy(
            prior.at[:, aligned(i, look)], seen.at[lax.rem(i, 2)], look_sem.at[lax.rem(i, 2)]
        )

    own = pltpu.make_async_copy(prior.at[:, aligned(me, width)], state.at[pl.ds(0, rows), :], own_sem)

    def there(k, c):
        column = pl.multiple_of((me ^ k) * width + c * span, span)
        return pltpu.make_async_remote_copy(
            src_ref=prior.at[:, pl.ds(column, span)],
            dst_ref=state.at[pl.ds(k * rows, rows), pl.ds(c * span, span)],
            send_sem=there_send,
            recv_sem=there_recv.at[c],
            device_id={"mem": me ^ k},
            device_id_type=MESH,
        )

    def back(k, c):
        column = pl.multiple_of(me * width + c * span, span)
        return pltpu.make_async_remote_copy(
            src_ref=state.at[pl.ds(k * rows, rows), pl.ds(c * span, span)],
            dst_ref=out.at[:, pl.ds(column, span)],
            send_sem=back_send,
            recv_sem=back_recv,
            device_id={"mem": me ^ k},
            device_id_type=MESH,
        )

    def along(d):
        return lax.rem(tile + d, tiles)

    def send_a(d):
        return pltpu.make_async_remote_copy(
            src_ref=pred_out.at[along(d)],
            dst_ref=pred_in.at[tile],
            send_sem=a_send,
            recv_sem=a_recv,
            device_id={"pix": along(d)},
            device_id_type=MESH,
        )

    def send_b(k):
        return pltpu.make_async_remote_copy(
            src_ref=mine,
            dst_ref=members_in.at[me],
            send_sem=b_send,
            recv_sem=b_recv,
            device_id={"mem": me ^ k},
            device_id_type=MESH,
        )

    def relay(k):
        return pltpu.make_async_remote_copy(
            src_ref=members_in.at[me ^ k],
            dst_ref=members_in.at[me ^ k],
            send_sem=r_send,
            recv_sem=r_recv,
            device_id={"mem": me ^ 1},
            device_id_type=MESH,
        )

    def send_c(d):
        return pltpu.make_async_remote_copy(
            src_ref=stats_in.at[tile],
            dst_ref=stats_in.at[tile],
            send_sem=c_send,
            recv_sem=c_recv,
            device_id={"pix": along(d)},
            device_id_type=MESH,
        )

    def whole(region, send_sem, recv_sem):
        return pltpu.make_async_remote_copy(
            src_ref=region,
            dst_ref=region,
            send_sem=send_sem,
            recv_sem=recv_sem,
            device_id={"mem": me ^ 1},
            device_id_type=MESH,
        )

    partners = list(reversed(range(1, parts)))
    evens = partners[1::2]
    others = list(range(1, tiles))

    barrier = pltpu.get_barrier_semaphore()
    for k in partners:
        pl.semaphore_signal(barrier, inc=1, device_id={"mem": me ^ k}, device_id_type=MESH)
    look_copy(0).start()
    for load in loads:
        load.start()

    speaker = me == parts - 1
    root = jnp.logical_and(speaker, tile == tiles - 1)
    branch = jnp.logical_and(speaker, tile != tiles - 1)

    @pl.when(jnp.logical_not(root))
    def _():
        pl.semaphore_wait(barrier, len(partners))

    @pl.when(branch)
    def _():
        root_id = {"mem": me, "pix": tiles - 1}
        pl.semaphore_signal(barrier, inc=1, device_id=root_id, device_id_type=MESH)

    @pl.when(root)
    def _():
        pl.semaphore_wait(barrier, len(partners) + len(others))
        for d in others:
            pl.semaphore_signal(go_sem, inc=1, device_id={"pix": along(d)}, device_id_type=MESH)
        for k in partners:
            pl.semaphore_signal(go_sem, inc=1, device_id={"mem": me ^ k}, device_id_type=MESH)

    for k in partners:
        there(k, 0).start()
    own.start()

    summer[...] = (iota((look, LANES), 0) // BLK == iota((look, LANES), 1)).astype(BF16)

    def look_step(i, carry):
        @pl.when(i + 1 < looks)
        def _():
            look_copy(i + 1).start()

        look_copy(i).wait()
        sums[:, aligned(i, LANES)] = jnp.dot(
            seen[lax.rem(i, 2)], summer[...], preferred_element_type=F32
        )
        return carry

    lax.fori_loop(0, looks, look_step, 0)

    for load in loads:
        load.wait()
    measured_row[...] = jnp.zeros((1, padded), F32)
    noise_row[...] = jnp.ones((1, padded), F32)
    early_row[...] = jnp.zeros((1, padded), jnp.int32)
    late_row[...] = jnp.zeros((1, padded), jnp.int32)
    target_row[...] = jnp.full((1, padded), -1, jnp.int32)
    measured_row[:, :obs] = measured_raw[...].reshape(1, obs)
    noise_row[:, :obs] = noise_raw[...].reshape(1, obs)
    early_row[:, :obs] = couples_raw[0:1, :]
    late_row[:, :obs] = couples_raw[1:2, :]
    target_row[:, :obs] = target_raw[...].reshape(1, obs) - tile * tile_blocks
    jitter_all[...] = jnp.zeros((PASS_COUNT, total_members, padded), F32)
    jitter_all[:, :, :obs] = jitter_raw[...]

    def predict(i, carry):
        lanes = aligned(i, share)
        table = (target_row[:, lanes] == iota((tile_blocks, share), 0)).astype(F32)
        part = nn(sums[...], table)
        scene = iota((rows, share), 0) % times
        pair = (scene == late_row[:, lanes]).astype(F32) - (scene == early_row[:, lanes]).astype(F32)
        group = (iota((members, rows), 1) // times == iota((members, rows), 0)).astype(F32)
        pred_out[i] = nn(group, part * pair) / BLK
        return carry

    lax.fori_loop(0, tiles, predict, 0)

    @pl.when(jnp.logical_not(root))
    def _():
        pl.semaphore_wait(go_sem, 1)

    @pl.when(branch)
    def _():
        for k in partners:
            pl.semaphore_signal(go_sem, inc=1, device_id={"mem": me ^ k}, device_id_type=MESH)

    for d in others:
        send_a(d).start()
    pred_in[tile] = pred_out[tile]
    whole(pred_in.at[pl.ds(0, len(others))], a_send, a_recv).wait()
    total = pred_in[0]
    for d in others:
        total = total + pred_in[d]
    mine[...] = total
    members_in[me] = total
    for k in evens + [1]:
        send_b(k).start()
    for c in range(1, CHUNKS):
        for k in partners:
            there(k, c).start()
    whole(members_in.at[pl.ds(0, len(evens) + 1)], b_send, b_recv).wait()
    for k in evens:
        relay(k).start()
    whole(members_in.at[pl.ds(0, len(evens))], r_send, r_recv).wait()

    pred = jnp.concatenate([members_in[i] for i in range(parts)], axis=0)
    lanes = aligned(tile, share)
    here = (iota((1, share), 1) + tile * share < obs).astype(F32)
    mean = jnp.mean(pred, axis=0, keepdims=True)
    scale = math.sqrt(float(PASS_COUNT)) * noise_row[:, lanes]
    centred = (pred - mean) / scale * here
    gap = jnp.broadcast_to((measured_row[:, lanes] - mean) / scale * here, pred.shape)
    stats_in[tile, 0] = nt(centred, jnp.concatenate([centred, gap], axis=0))
    shakes = jnp.concatenate([jitter_all[i, :, lanes] for i in range(PASS_COUNT)], axis=0)
    stats_in[tile, 1] = nt(centred, shakes)
    for d in others:
        send_c(d).start()
    whole(stats_in.at[pl.ds(0, len(others))], c_send, c_recv).wait()
    total = stats_in[0]
    for d in others:
        total = total + stats_in[d]

    expand(solve(total, work), me, parts, times, mix)

    own.wait()
    step = math.gcd(span, 256)
    depth = parts * rows
    for c in range(CHUNKS):
        arrived = state.at[pl.ds(rows, depth - rows), pl.ds(c * span, span)]
        whole(arrived, there_send, there_recv.at[c]).wait_recv()

        def update(i, carry):
            columns = pl.ds(pl.multiple_of(c * span + i * step, step), step)
            x = state[:, columns]
            both = jnp.dot(mix[...], x, preferred_element_type=F32)
            y = (x.astype(F32) + both[:depth] + both[depth:]).astype(BF16)
            state[:, columns] = y
            out[:, pl.ds(pl.multiple_of(me * width + c * span + i * step, step), step)] = y[:rows]
            return carry

        lax.fori_loop(0, span // step, update, 0)
        for k in partners:
            back(k, c).start()
    moved = state.at[pl.ds(rows, depth - rows), :]
    whole(moved, there_send, back_recv).wait_send()
    whole(moved, back_send, back_recv).wait()


def body(prior, measured, noise, jitter, couples, target):
    parts = lax.axis_size("mem")
    tiles = lax.axis_size("pix")
    members, times, cells = prior.shape
    total_members = members * parts
    rows = members * times
    depth = rows * parts
    width = cells // parts
    obs = target.shape[0]
    unit = LANES * tiles
    padded = obs + (-obs) % unit
    share = padded // tiles
    look = LANES * BLK
    far = pl.BlockSpec(memory_space=pltpu.HBM)
    dma = pltpu.SemaphoreType.DMA
    scratch = [
        pltpu.VMEM((depth, width), BF16),
        pltpu.VMEM((2 * depth, depth), BF16),
        pltpu.VMEM((2, rows, look), BF16),
        pltpu.VMEM((look, LANES), BF16),
        pltpu.VMEM((rows, cells // BLK), F32),
        pltpu.VMEM((total_members, 2 * total_members), F32),
        pltpu.VMEM((obs,), F32),
        pltpu.VMEM((obs,), F32),
        pltpu.VMEM((2, obs), jnp.int32),
        pltpu.VMEM((obs,), jnp.int32),
        pltpu.VMEM((PASS_COUNT, total_members, obs), F32),
        pltpu.VMEM((PASS_COUNT, total_members, padded), F32),
        pltpu.VMEM((1, padded), F32),
        pltpu.VMEM((1, padded), F32),
        pltpu.VMEM((1, padded), jnp.int32),
        pltpu.VMEM((1, padded), jnp.int32),
        pltpu.VMEM((1, padded), jnp.int32),
        pltpu.VMEM((tiles, members, share), F32),
        pltpu.VMEM((tiles, members, share), F32),
        pltpu.VMEM((members, share), F32),
        pltpu.VMEM((parts, members, share), F32),
        pltpu.VMEM((tiles, 2, total_members, 2 * total_members), F32),
        dma,
        dma((CHUNKS,)),
        dma,
        dma,
        dma,
        dma,
        dma,
        dma,
        dma,
        dma,
        dma,
        dma,
        dma((2,)),
        dma,
        dma((5,)),
        pltpu.SemaphoreType.REGULAR,
    ]
    operands = (
        prior.reshape(rows, cells),
        measured,
        noise,
        jnp.swapaxes(jitter, 1, 2),
        couples,
        target,
    )
    out = pl.pallas_call(
        functools.partial(smoother_kernel, parts, tiles, times),
        in_specs=[far] * 6,
        out_specs=pl.BlockSpec(memory_space=pltpu.VMEM),
        out_shape=pltpu.VMEM((rows, cells), BF16),
        scratch_shapes=scratch,
        compiler_params=pltpu.CompilerParams(
            collective_id=0, has_side_effects=True, vmem_limit_bytes=44 * 1024 * 1024
        ),
        name="smoother",
    )(*(pltpu.with_memory_space_constraint(a, pltpu.HBM) for a in operands))
    return out.reshape(prior.shape)


def solution(mesh):
    return jax.shard_map(
        body,
        mesh=mesh,
        in_specs=(P("mem", None, "pix"), P(), P(), P(), P(), P()),
        out_specs=P("mem", None, "pix"),
        check_vma=False,
    )
```

```python
import functools
import math

import jax
import jax.numpy as jnp
from jax import lax
from jax.experimental import pallas as pl
from jax.experimental.pallas import tpu as pltpu
from jax.sharding import PartitionSpec as P

BLK = 64
PASS_COUNT = 2
LANES = 128
CHUNKS = 4
F32 = jnp.float32
BF16 = jnp.bfloat16
HI = lax.Precision.HIGHEST
MESH = pl.DeviceIdType.MESH


def nn(a, b):
    return lax.dot_general(a, b, (((1,), (0,)), ((), ())), precision=HI, preferred_element_type=F32)


def tn(a, b):
    return nn(a.T, b)


def nt(a, b):
    return lax.dot_general(a, b, (((1,), (1,)), ((), ())), precision=HI, preferred_element_type=F32)


def iota(shape, axis):
    return lax.broadcasted_iota(jnp.int32, shape, axis)


def aligned(index, unit):
    return pl.ds(pl.multiple_of(index * unit, unit), unit)


def gauss_jordan(matrix, right, work):
    n = matrix.shape[0]
    work[...] = jnp.concatenate([matrix, right], axis=1)
    row_id = iota((n, 1), 0)
    lane_id = iota((n, 2 * n), 1)

    def step(k, carry):
        table = work[...]
        row = work[pl.ds(k, 1), :]
        here = lane_id == k
        factor = jnp.sum(jnp.where(here, table, 0.0), axis=1, keepdims=True)
        pivot = row / jnp.sum(jnp.where(here[:1], row, 0.0), axis=1, keepdims=True)
        work[...] = jnp.where(row_id == k, pivot, table - factor * pivot)
        return carry

    lax.fori_loop(0, n, step, 0)
    return work[:, n:]


def solve(total, work):
    n = total[0].shape[0]
    s, g = total[0][:, :n], total[0][:, n:]
    h1, h2 = total[1][:, :n], total[1][:, n:]
    eye = (iota((n, n), 0) == iota((n, n), 1)).astype(F32)
    m1 = gauss_jordan(eye + s / (n - 1), (g + h1 - s) / (n - 1), work).astype(BF16).astype(F32)
    m1_mean = jnp.mean(m1, axis=1, keepdims=True)
    step = eye + m1 - m1_mean
    s2 = tn(step, nn(s, step))
    g2 = tn(step, g - nn(s, jnp.broadcast_to(m1_mean, (n, n))))
    h22 = tn(step, h2)
    m2 = gauss_jordan(eye + s2 / (n - 1), (g2 + h22 - s2) / (n - 1), work).astype(BF16).astype(F32)
    m2c = m2 - jnp.mean(m2, axis=0, keepdims=True)
    w = m1 + m2 + nn(m1, m2c)
    return w - jnp.mean(w, axis=0, keepdims=True)


def expand(w, me, parts, times, mix):
    n = w.shape[0]
    members = n // parts
    rows = members * times
    depth = rows * parts
    spot = iota((n, n), 0)
    source = ((spot // members) ^ me) * members + spot % members
    order = (iota((n, n), 1) == source).astype(F32)
    wt = nt(nn(order, w.T), order)
    hi = wt.astype(BF16)
    lo = (wt - hi.astype(F32)).astype(BF16)
    spread = (iota((n, depth), 1) // times == iota((n, depth), 0)).astype(BF16)
    tall = (iota((rows, members), 0) // times == iota((rows, members), 1)).astype(BF16)
    same = iota((rows, depth), 0) % times == iota((rows, depth), 1) % times
    for piece, first in ((hi, 0), (lo, depth)):
        wide = jnp.dot(piece, spread, preferred_element_type=F32).astype(BF16)
        for part in range(parts):
            block = jnp.dot(
                tall, wide[part * members : (part + 1) * members, :], preferred_element_type=F32
            )
            start = first + part * rows
            mix[start : start + rows, :] = jnp.where(same, block, 0.0).astype(BF16)


def smoother_kernel(
    parts, tiles, times,
    prior, measured, noise, jitter, couples, target, out, rest, last,
    state, mix, seen, summer, sums, work,
    measured_raw, noise_raw, couples_raw, target_raw, jitter_raw, jitter_all,
    measured_row, noise_row, early_row, late_row, target_row,
    pred_out, pred_in, mine, members_in, stats_in,
    there_send, there_recv, back_send, back_recv, early_send, early_recv,
    a_send, a_recv, b_send, b_recv, r_send, r_recv, c_send, c_recv,
    look_sem, own_sem, small_sem, go_sem,
):
    me = lax.axis_index("mem")
    tile = lax.axis_index("pix")
    rows, cells = prior.shape
    members = rows // times
    total_members = members * parts
    width = cells // parts
    span = width // CHUNKS
    obs = target.shape[0]
    padded = target_row.shape[1]
    share = padded // tiles
    tile_blocks = cells // BLK
    look = seen.shape[2]
    looks = cells // look

    def small(i, source, dest):
        return pltpu.make_async_copy(source, dest, small_sem.at[i])

    loads = [
        small(0, measured, measured_raw),
        small(1, noise, noise_raw),
        small(2, couples, couples_raw),
        small(3, target, target_raw),
        small(4, jitter, jitter_raw),
    ]

    def look_copy(i):
        return pltpu.make_async_copy(
            prior.at[:, aligned(i, look)], seen.at[lax.rem(i, 2)], look_sem.at[lax.rem(i, 2)]
        )

    own = pltpu.make_async_copy(prior.at[:, aligned(me, width)], state.at[pl.ds(0, rows), :], own_sem)

    def there(k, c):
        column = pl.multiple_of((me ^ k) * width + c * span, span)
        return pltpu.make_async_remote_copy(
            src_ref=prior.at[:, pl.ds(column, span)],
            dst_ref=state.at[pl.ds(k * rows, rows), pl.ds(c * span, span)],
            send_sem=there_send,
            recv_sem=there_recv.at[c],
            device_id={"mem": me ^ k},
            device_id_type=MESH,
        )

    def back(k, c):
        column = pl.multiple_of(me * (width - span) + c * span, span)
        return pltpu.make_async_remote_copy(
            src_ref=state.at[pl.ds(k * rows, rows), pl.ds(c * span, span)],
            dst_ref=out.at[:, pl.ds(column, span)],
            send_sem=back_send,
            recv_sem=back_recv,
            device_id={"mem": me ^ k},
            device_id_type=MESH,
        )

    def early(k):
        return pltpu.make_async_remote_copy(
            src_ref=last.at[pl.ds(k * rows, rows), :],
            dst_ref=rest.at[:, aligned(me, span)],
            send_sem=early_send,
            recv_sem=early_recv,
            device_id={"mem": me ^ k},
            device_id_type=MESH,
        )

    def along(d):
        return lax.rem(tile + d, tiles)

    def send_a(d):
        return pltpu.make_async_remote_copy(
            src_ref=pred_out.at[along(d)],
            dst_ref=pred_in.at[tile],
            send_sem=a_send,
            recv_sem=a_recv,
            device_id={"pix": along(d)},
            device_id_type=MESH,
        )

    def send_b(k):
        return pltpu.make_async_remote_copy(
            src_ref=mine,
            dst_ref=members_in.at[me],
            send_sem=b_send,
            recv_sem=b_recv,
            device_id={"mem": me ^ k},
            device_id_type=MESH,
        )

    def relay(k):
        return pltpu.make_async_remote_copy(
            src_ref=members_in.at[me ^ k],
            dst_ref=members_in.at[me ^ k],
            send_sem=r_send,
            recv_sem=r_recv,
            device_id={"mem": me ^ 1},
            device_id_type=MESH,
        )

    def send_c(d):
        return pltpu.make_async_remote_copy(
            src_ref=stats_in.at[tile],
            dst_ref=stats_in.at[tile],
            send_sem=c_send,
            recv_sem=c_recv,
            device_id={"pix": along(d)},
            device_id_type=MESH,
        )

    def whole(region, send_sem, recv_sem):
        return pltpu.make_async_remote_copy(
            src_ref=region,
            dst_ref=region,
            send_sem=send_sem,
            recv_sem=recv_sem,
            device_id={"mem": me ^ 1},
            device_id_type=MESH,
        )

    partners = list(reversed(range(1, parts)))
    evens = partners[1::2]
    others = list(range(1, tiles))

    barrier = pltpu.get_barrier_semaphore()
    for k in partners:
        pl.semaphore_signal(barrier, inc=1, device_id={"mem": me ^ k}, device_id_type=MESH)
    look_copy(0).start()
    for load in loads:
        load.start()

    speaker = me == parts - 1
    root = jnp.logical_and(speaker, tile == tiles - 1)
    branch = jnp.logical_and(speaker, tile != tiles - 1)

    @pl.when(jnp.logical_not(root))
    def _():
        pl.semaphore_wait(barrier, len(partners))

    @pl.when(branch)
    def _():
        root_id = {"mem": me, "pix": tiles - 1}
        pl.semaphore_signal(barrier, inc=1, device_id=root_id, device_id_type=MESH)

    @pl.when(root)
    def _():
        pl.semaphore_wait(barrier, len(partners) + len(others))
        for d in others:
            pl.semaphore_signal(go_sem, inc=1, device_id={"pix": along(d)}, device_id_type=MESH)
        for k in partners:
            pl.semaphore_signal(go_sem, inc=1, device_id={"mem": me ^ k}, device_id_type=MESH)

    for k in partners:
        there(k, 0).start()
    own.start()

    summer[...] = (iota((look, LANES), 0) // BLK == iota((look, LANES), 1)).astype(BF16)

    def look_step(i, carry):
        @pl.when(i + 1 < looks)
        def _():
            look_copy(i + 1).start()

        look_copy(i).wait()
        sums[:, aligned(i, LANES)] = jnp.dot(
            seen[lax.rem(i, 2)], summer[...], preferred_element_type=F32
        )
        return carry

    lax.fori_loop(0, looks, look_step, 0)

    for load in loads:
        load.wait()
    measured_row[...] = jnp.zeros((1, padded), F32)
    noise_row[...] = jnp.ones((1, padded), F32)
    early_row[...] = jnp.zeros((1, padded), jnp.int32)
    late_row[...] = jnp.zeros((1, padded), jnp.int32)
    target_row[...] = jnp.full((1, padded), -1, jnp.int32)
    measured_row[:, :obs] = measured_raw[...].reshape(1, obs)
    noise_row[:, :obs] = noise_raw[...].reshape(1, obs)
    early_row[:, :obs] = couples_raw[0:1, :]
    late_row[:, :obs] = couples_raw[1:2, :]
    target_row[:, :obs] = target_raw[...].reshape(1, obs) - tile * tile_blocks
    jitter_all[...] = jnp.zeros((PASS_COUNT, total_members, padded), F32)
    jitter_all[:, :, :obs] = jitter_raw[...]

    def predict(i, carry):
        lanes = aligned(i, share)
        table = (target_row[:, lanes] == iota((tile_blocks, share), 0)).astype(F32)
        part = nn(sums[...], table)
        scene = iota((rows, share), 0) % times
        pair = (scene == late_row[:, lanes]).astype(F32) - (scene == early_row[:, lanes]).astype(F32)
        group = (iota((members, rows), 1) // times == iota((members, rows), 0)).astype(F32)
        pred_out[i] = nn(group, part * pair) / BLK
        return carry

    lax.fori_loop(0, tiles, predict, 0)

    @pl.when(jnp.logical_not(root))
    def _():
        pl.semaphore_wait(go_sem, 1)

    @pl.when(branch)
    def _():
        for k in partners:
            pl.semaphore_signal(go_sem, inc=1, device_id={"mem": me ^ k}, device_id_type=MESH)

    for d in others:
        send_a(d).start()
    pred_in[tile] = pred_out[tile]
    whole(pred_in.at[pl.ds(0, len(others))], a_send, a_recv).wait()
    total = pred_in[0]
    for d in others:
        total = total + pred_in[d]
    mine[...] = total
    members_in[me] = total
    for k in evens + [1]:
        send_b(k).start()
    for c in range(1, CHUNKS):
        for k in partners:
            there(k, c).start()
    whole(members_in.at[pl.ds(0, len(evens) + 1)], b_send, b_recv).wait()
    for k in evens:
        relay(k).start()
    whole(members_in.at[pl.ds(0, len(evens))], r_send, r_recv).wait()

    pred = jnp.concatenate([members_in[i] for i in range(parts)], axis=0)
    lanes = aligned(tile, share)
    here = (iota((1, share), 1) + tile * share < obs).astype(F32)
    mean = jnp.mean(pred, axis=0, keepdims=True)
    scale = math.sqrt(float(PASS_COUNT)) * noise_row[:, lanes]
    centred = (pred - mean) / scale * here
    gap = jnp.broadcast_to((measured_row[:, lanes] - mean) / scale * here, pred.shape)
    stats_in[tile, 0] = nt(centred, jnp.concatenate([centred, gap], axis=0))
    shakes = jnp.concatenate([jitter_all[i, :, lanes] for i in range(PASS_COUNT)], axis=0)
    stats_in[tile, 1] = nt(centred, shakes)
    for d in others:
        send_c(d).start()
    whole(stats_in.at[pl.ds(0, len(others))], c_send, c_recv).wait()
    total = stats_in[0]
    for d in others:
        total = total + stats_in[d]

    expand(solve(total, work), me, parts, times, mix)

    own.wait()
    step = math.gcd(span, 256)
    depth = parts * rows
    for c in range(CHUNKS):
        arrived = state.at[pl.ds(rows, depth - rows), pl.ds(c * span, span)]
        whole(arrived, there_send, there_recv.at[c]).wait_recv()

        def update(i, carry):
            columns = pl.ds(pl.multiple_of(c * span + i * step, step), step)
            x = state[:, columns]
            both = jnp.dot(mix[...], x, preferred_element_type=F32)
            y = (x.astype(F32) + both[:depth] + both[depth:]).astype(BF16)
            if c < CHUNKS - 1:
                state[:, columns] = y
                column = me * (width - span) + c * span + i * step
                out[:, pl.ds(pl.multiple_of(column, step), step)] = y[:rows]
            else:
                last[:, aligned(i, step)] = y
                rest[:, pl.ds(pl.multiple_of(me * span + i * step, step), step)] = y[:rows]
            return carry

        lax.fori_loop(0, span // step, update, 0)
        if c < CHUNKS - 1:
            for k in partners:
                back(k, c).start()

    odd = lax.rem(me, 2) == 1

    @pl.when(odd)
    def _():
        for k in evens:
            early(k).start()

    whole(state.at[pl.ds(rows, depth - rows), :], there_send, back_recv).wait_send()
    moved = state.at[pl.ds(rows, depth - rows), pl.ds(0, width - span)]
    whole(moved, back_send, back_recv).wait()

    @pl.when(odd)
    def _():
        whole(last.at[pl.ds(0, len(evens) * rows), :], early_send, early_recv).wait()


def finish_kernel(parts, out_early, rest, last, out, send_sem, recv_sem, go_sem):
    me = lax.axis_index("mem")
    rows = rest.shape[0]
    span = last.shape[1]
    partners = list(reversed(range(1, parts)))
    evens = partners[1::2]
    odds = partners[0::2]
    odd = lax.rem(me, 2) == 1
    even = jnp.logical_not(odd)
    barrier = pltpu.get_barrier_semaphore()

    def copy(k):
        return pltpu.make_async_remote_copy(
            src_ref=last.at[pl.ds(k * rows, rows), :],
            dst_ref=out.at[:, aligned(me, span)],
            send_sem=send_sem,
            recv_sem=recv_sem,
            device_id={"mem": me ^ k},
            device_id_type=MESH,
        )

    def signal(sem, k):
        pl.semaphore_signal(sem, inc=1, device_id={"mem": me ^ k}, device_id_type=MESH)

    def settle(count):
        region = last.at[pl.ds(0, count * rows), :]
        pltpu.make_async_remote_copy(
            src_ref=region,
            dst_ref=region,
            send_sem=send_sem,
            recv_sem=recv_sem,
            device_id={"mem": me ^ 1},
            device_id_type=MESH,
        ).wait()

    for k in evens:
        signal(barrier, k)

    @pl.when(even)
    def _():
        for k in odds:
            signal(barrier, k)
        pl.semaphore_wait(barrier, len(evens))
        for k in evens:
            copy(k).start()
        pl.semaphore_wait(go_sem, len(odds))

    @pl.when(odd)
    def _():
        pl.semaphore_wait(barrier, len(partners))
        for k in odds:
            signal(go_sem, k)

    for k in odds:
        copy(k).start()
    out[:, aligned(me, span)] = rest[:, aligned(me, span)]

    @pl.when(odd)
    def _():
        for k in evens:
            out[:, aligned(me ^ k, span)] = rest[:, aligned(me ^ k, span)]
        settle(len(odds))

    @pl.when(even)
    def _():
        settle(len(partners))


def write_kernel(parts, width, offset, piece, out, sem):
    size = piece.shape[1] // parts
    copies = [
        pltpu.make_async_copy(
            piece.at[:, pl.ds(i * size, size)],
            out.at[:, pl.ds(i * width + offset, size)],
            sem.at[i],
        )
        for i in range(parts)
    ]
    for copy in copies:
        copy.start()
    for copy in copies:
        copy.wait()


def body(prior, measured, noise, jitter, couples, target):
    parts = lax.axis_size("mem")
    tiles = lax.axis_size("pix")
    members, times, cells = prior.shape
    total_members = members * parts
    rows = members * times
    depth = rows * parts
    width = cells // parts
    obs = target.shape[0]
    unit = LANES * tiles
    padded = obs + (-obs) % unit
    share = padded // tiles
    look = LANES * BLK
    far = pl.BlockSpec(memory_space=pltpu.HBM)
    dma = pltpu.SemaphoreType.DMA
    scratch = [
        pltpu.VMEM((depth, width), BF16),
        pltpu.VMEM((2 * depth, depth), BF16),
        pltpu.VMEM((2, rows, look), BF16),
        pltpu.VMEM((look, LANES), BF16),
        pltpu.VMEM((rows, cells // BLK), F32),
        pltpu.VMEM((total_members, 2 * total_members), F32),
        pltpu.VMEM((obs,), F32),
        pltpu.VMEM((obs,), F32),
        pltpu.VMEM((2, obs), jnp.int32),
        pltpu.VMEM((obs,), jnp.int32),
        pltpu.VMEM((PASS_COUNT, total_members, obs), F32),
        pltpu.VMEM((PASS_COUNT, total_members, padded), F32),
        pltpu.VMEM((1, padded), F32),
        pltpu.VMEM((1, padded), F32),
        pltpu.VMEM((1, padded), jnp.int32),
        pltpu.VMEM((1, padded), jnp.int32),
        pltpu.VMEM((1, padded), jnp.int32),
        pltpu.VMEM((tiles, members, share), F32),
        pltpu.VMEM((tiles, members, share), F32),
        pltpu.VMEM((members, share), F32),
        pltpu.VMEM((parts, members, share), F32),
        pltpu.VMEM((tiles, 2, total_members, 2 * total_members), F32),
        dma,
        dma((CHUNKS,)),
        dma,
        dma,
        dma,
        dma,
        dma,
        dma,
        dma,
        dma,
        dma,
        dma,
        dma,
        dma,
        dma((2,)),
        dma,
        dma((5,)),
        pltpu.SemaphoreType.REGULAR,
    ]
    operands = (
        prior.reshape(rows, cells),
        measured,
        noise,
        jnp.swapaxes(jitter, 1, 2),
        couples,
        target,
    )
    span = width // CHUNKS
    near = pl.BlockSpec(memory_space=pltpu.VMEM)
    most, rest, last = pl.pallas_call(
        functools.partial(smoother_kernel, parts, tiles, times),
        in_specs=[far] * 6,
        out_specs=[near] * 3,
        out_shape=[
            pltpu.VMEM((rows, parts * (width - span)), BF16),
            pltpu.VMEM((rows, parts * span), BF16),
            pltpu.VMEM((depth, span), BF16),
        ],
        scratch_shapes=scratch,
        compiler_params=pltpu.CompilerParams(
            collective_id=0, has_side_effects=True, vmem_limit_bytes=44 * 1024 * 1024
        ),
        name="smoother",
    )(*(pltpu.with_memory_space_constraint(a, pltpu.HBM) for a in operands))
    out = pl.pallas_call(
        functools.partial(write_kernel, parts, width, 0),
        in_specs=[near],
        out_specs=far,
        out_shape=pltpu.HBM((rows, cells), BF16),
        scratch_shapes=[dma((parts,))],
        compiler_params=pltpu.CompilerParams(vmem_limit_bytes=4 * 1024 * 1024),
        name="write_most",
    )(most)
    rest = pl.pallas_call(
        functools.partial(finish_kernel, parts),
        in_specs=[far, near, near],
        out_specs=near,
        out_shape=pltpu.VMEM((rows, parts * span), BF16),
        scratch_shapes=[dma, dma, pltpu.SemaphoreType.REGULAR],
        compiler_params=pltpu.CompilerParams(
            collective_id=1, has_side_effects=True, vmem_limit_bytes=8 * 1024 * 1024
        ),
        name="finish",
    )(pltpu.with_memory_space_constraint(out, pltpu.HBM), rest, last)

    def write_rest(piece, before, after, sem):
        write_kernel(parts, width, width - span, piece, after, sem)

    out = pl.pallas_call(
        write_rest,
        in_specs=[near, far],
        out_specs=far,
        out_shape=pltpu.HBM((rows, cells), BF16),
        input_output_aliases={1: 0},
        scratch_shapes=[dma((parts,))],
        compiler_params=pltpu.CompilerParams(vmem_limit_bytes=4 * 1024 * 1024),
        name="write_rest",
    )(rest, out)
    return out.reshape(prior.shape)


def solution(mesh):
    return jax.shard_map(
        body,
        mesh=mesh,
        in_specs=(P("mem", None, "pix"), P(), P(), P(), P(), P()),
        out_specs=P("mem", None, "pix"),
        check_vma=False,
    )
```

```python
import functools
import math

import jax
import jax.numpy as jnp
from jax import lax
from jax.experimental import pallas as pl
from jax.experimental.pallas import tpu as pltpu
from jax.sharding import PartitionSpec as P

BLK = 64
PASS_COUNT = 2
LANES = 128
SHARES = (4, 4, 3, 5)
CHUNKS = len(SHARES)
F32 = jnp.float32
BF16 = jnp.bfloat16
HI = lax.Precision.HIGHEST
MESH = pl.DeviceIdType.MESH


def nn(a, b):
    return lax.dot_general(a, b, (((1,), (0,)), ((), ())), precision=HI, preferred_element_type=F32)


def tn(a, b):
    return nn(a.T, b)


def nt(a, b):
    return lax.dot_general(a, b, (((1,), (1,)), ((), ())), precision=HI, preferred_element_type=F32)


def iota(shape, axis):
    return lax.broadcasted_iota(jnp.int32, shape, axis)


def aligned(index, unit):
    return pl.ds(pl.multiple_of(index * unit, unit), unit)


def spans(width):
    return [width * part // sum(SHARES) for part in SHARES]


def gauss_jordan(matrix, right, work):
    n = matrix.shape[0]
    work[...] = jnp.concatenate([matrix, right], axis=1)
    row_id = iota((n, 1), 0)
    lane_id = iota((n, 2 * n), 1)

    def step(k, carry):
        table = work[...]
        row = work[pl.ds(k, 1), :]
        here = lane_id == k
        factor = jnp.sum(jnp.where(here, table, 0.0), axis=1, keepdims=True)
        pivot = row / jnp.sum(jnp.where(here[:1], row, 0.0), axis=1, keepdims=True)
        work[...] = jnp.where(row_id == k, pivot, table - factor * pivot)
        return carry

    lax.fori_loop(0, n, step, 0)
    return work[:, n:]


def solve(total, work):
    n = total[0].shape[0]
    s, g = total[0][:, :n], total[0][:, n:]
    h1, h2 = total[1][:, :n], total[1][:, n:]
    eye = (iota((n, n), 0) == iota((n, n), 1)).astype(F32)
    m1 = gauss_jordan(eye + s / (n - 1), (g + h1 - s) / (n - 1), work).astype(BF16).astype(F32)
    m1_mean = jnp.mean(m1, axis=1, keepdims=True)
    step = eye + m1 - m1_mean
    s2 = tn(step, nn(s, step))
    g2 = tn(step, g - nn(s, jnp.broadcast_to(m1_mean, (n, n))))
    h22 = tn(step, h2)
    m2 = gauss_jordan(eye + s2 / (n - 1), (g2 + h22 - s2) / (n - 1), work).astype(BF16).astype(F32)
    m2c = m2 - jnp.mean(m2, axis=0, keepdims=True)
    w = m1 + m2 + nn(m1, m2c)
    return w - jnp.mean(w, axis=0, keepdims=True)


def expand(w, me, parts, times, mix):
    n = w.shape[0]
    members = n // parts
    rows = members * times
    depth = rows * parts
    spot = iota((n, n), 0)
    source = ((spot // members) ^ me) * members + spot % members
    order = (iota((n, n), 1) == source).astype(F32)
    wt = nt(nn(order, w.T), order)
    hi = wt.astype(BF16)
    lo = (wt - hi.astype(F32)).astype(BF16)
    spread = (iota((n, depth), 1) // times == iota((n, depth), 0)).astype(BF16)
    tall = (iota((rows, members), 0) // times == iota((rows, members), 1)).astype(BF16)
    same = iota((rows, depth), 0) % times == iota((rows, depth), 1) % times
    for piece, first in ((hi, 0), (lo, depth)):
        wide = jnp.dot(piece, spread, preferred_element_type=F32).astype(BF16)
        for part in range(parts):
            block = jnp.dot(
                tall, wide[part * members : (part + 1) * members, :], preferred_element_type=F32
            )
            start = first + part * rows
            mix[start : start + rows, :] = jnp.where(same, block, 0.0).astype(BF16)


def smoother_kernel(
    parts, tiles, times,
    prior, measured, noise, jitter, couples, target, out, rest, last,
    state, mix, seen, summer, sums, work,
    measured_raw, noise_raw, couples_raw, target_raw, jitter_raw, jitter_all,
    measured_row, noise_row, early_row, late_row, target_row,
    pred_out, pred_in, mine, members_in, stats_in,
    there_send, there_recv, back_send, back_recv, early_send, early_recv,
    a_send, a_recv, b_send, b_recv, r_send, r_recv, c_send, c_recv,
    look_sem, own_sem, small_sem, go_sem,
):
    me = lax.axis_index("mem")
    tile = lax.axis_index("pix")
    rows, cells = prior.shape
    members = rows // times
    total_members = members * parts
    width = cells // parts
    size = spans(width)
    first = [sum(size[:c]) for c in range(CHUNKS)]
    tail = size[-1]
    obs = target.shape[0]
    padded = target_row.shape[1]
    share = padded // tiles
    tile_blocks = cells // BLK
    look = seen.shape[2]
    looks = cells // look

    def small(i, source, dest):
        return pltpu.make_async_copy(source, dest, small_sem.at[i])

    loads = [
        small(0, measured, measured_raw),
        small(1, noise, noise_raw),
        small(2, couples, couples_raw),
        small(3, target, target_raw),
        small(4, jitter, jitter_raw),
    ]

    def look_copy(i):
        return pltpu.make_async_copy(
            prior.at[:, aligned(i, look)], seen.at[lax.rem(i, 2)], look_sem.at[lax.rem(i, 2)]
        )

    own = pltpu.make_async_copy(prior.at[:, aligned(me, width)], state.at[pl.ds(0, rows), :], own_sem)

    def there(k, c):
        column = pl.multiple_of((me ^ k) * width + first[c], LANES)
        return pltpu.make_async_remote_copy(
            src_ref=prior.at[:, pl.ds(column, size[c])],
            dst_ref=state.at[pl.ds(k * rows, rows), pl.ds(first[c], size[c])],
            send_sem=there_send,
            recv_sem=there_recv.at[c],
            device_id={"mem": me ^ k},
            device_id_type=MESH,
        )

    def back(k, c):
        column = pl.multiple_of(me * (width - tail) + first[c], LANES)
        return pltpu.make_async_remote_copy(
            src_ref=state.at[pl.ds(k * rows, rows), pl.ds(first[c], size[c])],
            dst_ref=out.at[:, pl.ds(column, size[c])],
            send_sem=back_send,
            recv_sem=back_recv,
            device_id={"mem": me ^ k},
            device_id_type=MESH,
        )

    def early(k):
        return pltpu.make_async_remote_copy(
            src_ref=last.at[pl.ds(k * rows, rows), :],
            dst_ref=rest.at[:, aligned(me, tail)],
            send_sem=early_send,
            recv_sem=early_recv,
            device_id={"mem": me ^ k},
            device_id_type=MESH,
        )

    def along(d):
        return lax.rem(tile + d, tiles)

    def send_a(d):
        return pltpu.make_async_remote_copy(
            src_ref=pred_out.at[along(d)],
            dst_ref=pred_in.at[tile],
            send_sem=a_send,
            recv_sem=a_recv,
            device_id={"pix": along(d)},
            device_id_type=MESH,
        )

    def send_b(k):
        return pltpu.make_async_remote_copy(
            src_ref=mine,
            dst_ref=members_in.at[me],
            send_sem=b_send,
            recv_sem=b_recv,
            device_id={"mem": me ^ k},
            device_id_type=MESH,
        )

    def relay(k):
        return pltpu.make_async_remote_copy(
            src_ref=members_in.at[me ^ k],
            dst_ref=members_in.at[me ^ k],
            send_sem=r_send,
            recv_sem=r_recv,
            device_id={"mem": me ^ 1},
            device_id_type=MESH,
        )

    def send_c(d):
        return pltpu.make_async_remote_copy(
            src_ref=stats_in.at[tile],
            dst_ref=stats_in.at[tile],
            send_sem=c_send,
            recv_sem=c_recv,
            device_id={"pix": along(d)},
            device_id_type=MESH,
        )

    def whole(region, send_sem, recv_sem):
        return pltpu.make_async_remote_copy(
            src_ref=region,
            dst_ref=region,
            send_sem=send_sem,
            recv_sem=recv_sem,
            device_id={"mem": me ^ 1},
            device_id_type=MESH,
        )

    partners = list(reversed(range(1, parts)))
    evens = partners[1::2]
    others = list(range(1, tiles))

    barrier = pltpu.get_barrier_semaphore()
    for k in partners:
        pl.semaphore_signal(barrier, inc=1, device_id={"mem": me ^ k}, device_id_type=MESH)
    look_copy(0).start()
    for load in loads:
        load.start()

    speaker = me == parts - 1
    root = jnp.logical_and(speaker, tile == tiles - 1)
    branch = jnp.logical_and(speaker, tile != tiles - 1)

    @pl.when(jnp.logical_not(root))
    def _():
        pl.semaphore_wait(barrier, len(partners))

    @pl.when(branch)
    def _():
        root_id = {"mem": me, "pix": tiles - 1}
        pl.semaphore_signal(barrier, inc=1, device_id=root_id, device_id_type=MESH)

    @pl.when(root)
    def _():
        pl.semaphore_wait(barrier, len(partners) + len(others))
        for d in others:
            pl.semaphore_signal(go_sem, inc=1, device_id={"pix": along(d)}, device_id_type=MESH)
        for k in partners:
            pl.semaphore_signal(go_sem, inc=1, device_id={"mem": me ^ k}, device_id_type=MESH)

    for k in partners:
        there(k, 0).start()
    own.start()

    summer[...] = (iota((look, LANES), 0) // BLK == iota((look, LANES), 1)).astype(BF16)

    def look_step(i, carry):
        @pl.when(i + 1 < looks)
        def _():
            look_copy(i + 1).start()

        look_copy(i).wait()
        sums[:, aligned(i, LANES)] = jnp.dot(
            seen[lax.rem(i, 2)], summer[...], preferred_element_type=F32
        )
        return carry

    lax.fori_loop(0, looks, look_step, 0)

    for load in loads:
        load.wait()
    measured_row[...] = jnp.zeros((1, padded), F32)
    noise_row[...] = jnp.ones((1, padded), F32)
    early_row[...] = jnp.zeros((1, padded), jnp.int32)
    late_row[...] = jnp.zeros((1, padded), jnp.int32)
    target_row[...] = jnp.full((1, padded), -1, jnp.int32)
    measured_row[:, :obs] = measured_raw[...].reshape(1, obs)
    noise_row[:, :obs] = noise_raw[...].reshape(1, obs)
    early_row[:, :obs] = couples_raw[0:1, :]
    late_row[:, :obs] = couples_raw[1:2, :]
    target_row[:, :obs] = target_raw[...].reshape(1, obs) - tile * tile_blocks
    jitter_all[...] = jnp.zeros((PASS_COUNT, total_members, padded), F32)
    jitter_all[:, :, :obs] = jitter_raw[...]

    def predict(i, carry):
        lanes = aligned(i, share)
        table = (target_row[:, lanes] == iota((tile_blocks, share), 0)).astype(F32)
        part = nn(sums[...], table)
        scene = iota((rows, share), 0) % times
        pair = (scene == late_row[:, lanes]).astype(F32) - (scene == early_row[:, lanes]).astype(F32)
        group = (iota((members, rows), 1) // times == iota((members, rows), 0)).astype(F32)
        pred_out[i] = nn(group, part * pair) / BLK
        return carry

    lax.fori_loop(0, tiles, predict, 0)

    @pl.when(jnp.logical_not(root))
    def _():
        pl.semaphore_wait(go_sem, 1)

    @pl.when(branch)
    def _():
        for k in partners:
            pl.semaphore_signal(go_sem, inc=1, device_id={"mem": me ^ k}, device_id_type=MESH)

    for d in others:
        send_a(d).start()
    pred_in[tile] = pred_out[tile]
    whole(pred_in.at[pl.ds(0, len(others))], a_send, a_recv).wait()
    total = pred_in[0]
    for d in others:
        total = total + pred_in[d]
    mine[...] = total
    members_in[me] = total
    for k in evens + [1]:
        send_b(k).start()
    for c in range(1, CHUNKS):
        for k in partners:
            there(k, c).start()
    whole(members_in.at[pl.ds(0, len(evens) + 1)], b_send, b_recv).wait()
    for k in evens:
        relay(k).start()
    whole(members_in.at[pl.ds(0, len(evens))], r_send, r_recv).wait()

    pred = jnp.concatenate([members_in[i] for i in range(parts)], axis=0)
    lanes = aligned(tile, share)
    here = (iota((1, share), 1) + tile * share < obs).astype(F32)
    mean = jnp.mean(pred, axis=0, keepdims=True)
    scale = math.sqrt(float(PASS_COUNT)) * noise_row[:, lanes]
    centred = (pred - mean) / scale * here
    gap = jnp.broadcast_to((measured_row[:, lanes] - mean) / scale * here, pred.shape)
    stats_in[tile, 0] = nt(centred, jnp.concatenate([centred, gap], axis=0))
    shakes = jnp.concatenate([jitter_all[i, :, lanes] for i in range(PASS_COUNT)], axis=0)
    stats_in[tile, 1] = nt(centred, shakes)
    for d in others:
        send_c(d).start()
    whole(stats_in.at[pl.ds(0, len(others))], c_send, c_recv).wait()
    total = stats_in[0]
    for d in others:
        total = total + stats_in[d]

    expand(solve(total, work), me, parts, times, mix)

    own.wait()
    step = math.gcd(256, *size)
    depth = parts * rows
    for c in range(CHUNKS):
        arrived = state.at[pl.ds(rows, depth - rows), pl.ds(first[c], size[c])]
        whole(arrived, there_send, there_recv.at[c]).wait_recv()

        def update(i, carry):
            columns = pl.ds(pl.multiple_of(first[c] + i * step, step), step)
            x = state[:, columns]
            both = jnp.dot(mix[...], x, preferred_element_type=F32)
            y = (x.astype(F32) + both[:depth] + both[depth:]).astype(BF16)
            if c < CHUNKS - 1:
                state[:, columns] = y
                column = me * (width - tail) + first[c] + i * step
                out[:, pl.ds(pl.multiple_of(column, step), step)] = y[:rows]
            else:
                last[:, aligned(i, step)] = y
                rest[:, pl.ds(pl.multiple_of(me * tail + i * step, step), step)] = y[:rows]
            return carry

        lax.fori_loop(0, size[c] // step, update, 0)
        if c < CHUNKS - 1:
            for k in partners:
                back(k, c).start()

    odd = lax.rem(me, 2) == 1

    @pl.when(odd)
    def _():
        for k in evens:
            early(k).start()

    whole(state.at[pl.ds(rows, depth - rows), :], there_send, back_recv).wait_send()
    moved = state.at[pl.ds(rows, depth - rows), pl.ds(0, width - tail)]
    whole(moved, back_send, back_recv).wait()

    @pl.when(odd)
    def _():
        whole(last.at[pl.ds(0, len(evens) * rows), :], early_send, early_recv).wait()


def finish_kernel(parts, out_early, rest, last, out, send_sem, recv_sem, go_sem):
    me = lax.axis_index("mem")
    rows = rest.shape[0]
    span = last.shape[1]
    partners = list(reversed(range(1, parts)))
    evens = partners[1::2]
    odds = partners[0::2]
    odd = lax.rem(me, 2) == 1
    even = jnp.logical_not(odd)
    barrier = pltpu.get_barrier_semaphore()

    def copy(k):
        return pltpu.make_async_remote_copy(
            src_ref=last.at[pl.ds(k * rows, rows), :],
            dst_ref=out.at[:, aligned(me, span)],
            send_sem=send_sem,
            recv_sem=recv_sem,
            device_id={"mem": me ^ k},
            device_id_type=MESH,
        )

    def signal(sem, k):
        pl.semaphore_signal(sem, inc=1, device_id={"mem": me ^ k}, device_id_type=MESH)

    def settle(count):
        region = last.at[pl.ds(0, count * rows), :]
        pltpu.make_async_remote_copy(
            src_ref=region,
            dst_ref=region,
            send_sem=send_sem,
            recv_sem=recv_sem,
            device_id={"mem": me ^ 1},
            device_id_type=MESH,
        ).wait()

    @pl.when(even)
    def _():
        for k in partners:
            signal(barrier, k)
        pl.semaphore_wait(barrier, len(evens))
        for k in evens:
            copy(k).start()
        pl.semaphore_wait(go_sem, len(odds))

    @pl.when(odd)
    def _():
        pl.semaphore_wait(barrier, len(odds))
        for k in odds:
            signal(go_sem, k)

    for k in odds:
        copy(k).start()
    out[:, aligned(me, span)] = rest[:, aligned(me, span)]

    @pl.when(odd)
    def _():
        for k in evens:
            out[:, aligned(me ^ k, span)] = rest[:, aligned(me ^ k, span)]
        settle(len(odds))

    @pl.when(even)
    def _():
        settle(len(partners))


def write_kernel(parts, width, offset, piece, out, sem):
    size = piece.shape[1] // parts
    copies = [
        pltpu.make_async_copy(
            piece.at[:, pl.ds(i * size, size)],
            out.at[:, pl.ds(i * width + offset, size)],
            sem.at[i],
        )
        for i in range(parts)
    ]
    for copy in copies:
        copy.start()
    for copy in copies:
        copy.wait()


def body(prior, measured, noise, jitter, couples, target):
    parts = lax.axis_size("mem")
    tiles = lax.axis_size("pix")
    members, times, cells = prior.shape
    total_members = members * parts
    rows = members * times
    depth = rows * parts
    width = cells // parts
    obs = target.shape[0]
    unit = LANES * tiles
    padded = obs + (-obs) % unit
    share = padded // tiles
    look = LANES * BLK
    far = pl.BlockSpec(memory_space=pltpu.HBM)
    dma = pltpu.SemaphoreType.DMA
    scratch = [
        pltpu.VMEM((depth, width), BF16),
        pltpu.VMEM((2 * depth, depth), BF16),
        pltpu.VMEM((2, rows, look), BF16),
        pltpu.VMEM((look, LANES), BF16),
        pltpu.VMEM((rows, cells // BLK), F32),
        pltpu.VMEM((total_members, 2 * total_members), F32),
        pltpu.VMEM((obs,), F32),
        pltpu.VMEM((obs,), F32),
        pltpu.VMEM((2, obs), jnp.int32),
        pltpu.VMEM((obs,), jnp.int32),
        pltpu.VMEM((PASS_COUNT, total_members, obs), F32),
        pltpu.VMEM((PASS_COUNT, total_members, padded), F32),
        pltpu.VMEM((1, padded), F32),
        pltpu.VMEM((1, padded), F32),
        pltpu.VMEM((1, padded), jnp.int32),
        pltpu.VMEM((1, padded), jnp.int32),
        pltpu.VMEM((1, padded), jnp.int32),
        pltpu.VMEM((tiles, members, share), F32),
        pltpu.VMEM((tiles, members, share), F32),
        pltpu.VMEM((members, share), F32),
        pltpu.VMEM((parts, members, share), F32),
        pltpu.VMEM((tiles, 2, total_members, 2 * total_members), F32),
        dma,
        dma((CHUNKS,)),
        dma,
        dma,
        dma,
        dma,
        dma,
        dma,
        dma,
        dma,
        dma,
        dma,
        dma,
        dma,
        dma((2,)),
        dma,
        dma((5,)),
        pltpu.SemaphoreType.REGULAR,
    ]
    operands = (
        prior.reshape(rows, cells),
        measured,
        noise,
        jnp.swapaxes(jitter, 1, 2),
        couples,
        target,
    )
    span = spans(width)[-1]
    near = pl.BlockSpec(memory_space=pltpu.VMEM)
    most, rest, last = pl.pallas_call(
        functools.partial(smoother_kernel, parts, tiles, times),
        in_specs=[far] * 6,
        out_specs=[near] * 3,
        out_shape=[
            pltpu.VMEM((rows, parts * (width - span)), BF16),
            pltpu.VMEM((rows, parts * span), BF16),
            pltpu.VMEM((depth, span), BF16),
        ],
        scratch_shapes=scratch,
        compiler_params=pltpu.CompilerParams(
            collective_id=0, has_side_effects=True, vmem_limit_bytes=44 * 1024 * 1024
        ),
        name="smoother",
    )(*(pltpu.with_memory_space_constraint(a, pltpu.HBM) for a in operands))
    out = pl.pallas_call(
        functools.partial(write_kernel, parts, width, 0),
        in_specs=[near],
        out_specs=far,
        out_shape=pltpu.HBM((rows, cells), BF16),
        scratch_shapes=[dma((parts,))],
        compiler_params=pltpu.CompilerParams(vmem_limit_bytes=4 * 1024 * 1024),
        name="write_most",
    )(most)
    rest = pl.pallas_call(
        functools.partial(finish_kernel, parts),
        in_specs=[far, near, near],
        out_specs=near,
        out_shape=pltpu.VMEM((rows, parts * span), BF16),
        scratch_shapes=[dma, dma, pltpu.SemaphoreType.REGULAR],
        compiler_params=pltpu.CompilerParams(
            collective_id=1, has_side_effects=True, vmem_limit_bytes=8 * 1024 * 1024
        ),
        name="finish",
    )(pltpu.with_memory_space_constraint(out, pltpu.HBM), rest, last)

    def write_rest(piece, before, after, sem):
        write_kernel(parts, width, width - span, piece, after, sem)

    out = pl.pallas_call(
        write_rest,
        in_specs=[near, far],
        out_specs=far,
        out_shape=pltpu.HBM((rows, cells), BF16),
        input_output_aliases={1: 0},
        scratch_shapes=[dma((parts,))],
        compiler_params=pltpu.CompilerParams(vmem_limit_bytes=4 * 1024 * 1024),
        name="write_rest",
    )(rest, out)
    return out.reshape(prior.shape)


def solution(mesh):
    return jax.shard_map(
        body,
        mesh=mesh,
        in_specs=(P("mem", None, "pix"), P(), P(), P(), P(), P()),
        out_specs=P("mem", None, "pix"),
        check_vma=False,
    )
```

```python
import functools
import math

import jax
import jax.numpy as jnp
from jax import lax
from jax.experimental import pallas as pl
from jax.experimental.pallas import tpu as pltpu
from jax.sharding import PartitionSpec as P

BLK = 64
PASS_COUNT = 2
LANES = 128
SHARES = (4, 4, 3, 5)
CHUNKS = len(SHARES)
F32 = jnp.float32
BF16 = jnp.bfloat16
HI = lax.Precision.HIGHEST
MESH = pl.DeviceIdType.MESH


def nn(a, b):
    return lax.dot_general(a, b, (((1,), (0,)), ((), ())), precision=HI, preferred_element_type=F32)


def tn(a, b):
    return nn(a.T, b)


def nt(a, b):
    return lax.dot_general(a, b, (((1,), (1,)), ((), ())), precision=HI, preferred_element_type=F32)


def iota(shape, axis):
    return lax.broadcasted_iota(jnp.int32, shape, axis)


def aligned(index, unit):
    return pl.ds(pl.multiple_of(index * unit, unit), unit)


def spans(width):
    return [width * part // sum(SHARES) for part in SHARES]


def gauss_jordan(matrix, right, work):
    n = matrix.shape[0]
    work[...] = jnp.concatenate([matrix, right], axis=1)
    row_id = iota((n, 1), 0)
    lane_id = iota((n, 2 * n), 1)

    def step(k, carry):
        table = work[...]
        row = work[pl.ds(k, 1), :]
        here = lane_id == k
        factor = jnp.sum(jnp.where(here, table, 0.0), axis=1, keepdims=True)
        pivot = row / jnp.sum(jnp.where(here[:1], row, 0.0), axis=1, keepdims=True)
        work[...] = jnp.where(row_id == k, pivot, table - factor * pivot)
        return carry

    lax.fori_loop(0, n, step, 0)
    return work[:, n:]


def solve(total, work):
    n = total[0].shape[0]
    s, g = total[0][:, :n], total[0][:, n:]
    h1, h2 = total[1][:, :n], total[1][:, n:]
    eye = (iota((n, n), 0) == iota((n, n), 1)).astype(F32)
    m1 = gauss_jordan(eye + s / (n - 1), (g + h1 - s) / (n - 1), work).astype(BF16).astype(F32)
    m1_mean = jnp.mean(m1, axis=1, keepdims=True)
    step = eye + m1 - m1_mean
    s2 = tn(step, nn(s, step))
    g2 = tn(step, g - nn(s, jnp.broadcast_to(m1_mean, (n, n))))
    h22 = tn(step, h2)
    m2 = gauss_jordan(eye + s2 / (n - 1), (g2 + h22 - s2) / (n - 1), work).astype(BF16).astype(F32)
    m2c = m2 - jnp.mean(m2, axis=0, keepdims=True)
    w = m1 + m2 + nn(m1, m2c)
    return w - jnp.mean(w, axis=0, keepdims=True)


def expand(w, me, parts, times, mix):
    n = w.shape[0]
    members = n // parts
    rows = members * times
    depth = rows * parts
    spot = iota((n, n), 0)
    source = ((spot // members) ^ me) * members + spot % members
    order = (iota((n, n), 1) == source).astype(F32)
    wt = nt(nn(order, w.T), order)
    hi = wt.astype(BF16)
    lo = (wt - hi.astype(F32)).astype(BF16)
    spread = (iota((n, depth), 1) // times == iota((n, depth), 0)).astype(BF16)
    tall = (iota((rows, members), 0) // times == iota((rows, members), 1)).astype(BF16)
    same = iota((rows, depth), 0) % times == iota((rows, depth), 1) % times
    for piece, first in ((hi, 0), (lo, depth)):
        wide = jnp.dot(piece, spread, preferred_element_type=F32).astype(BF16)
        for part in range(parts):
            block = jnp.dot(
                tall, wide[part * members : (part + 1) * members, :], preferred_element_type=F32
            )
            start = first + part * rows
            mix[start : start + rows, :] = jnp.where(same, block, 0.0).astype(BF16)


def smoother_kernel(
    parts, tiles, times,
    prior, measured, noise, jitter, couples, target, out, rest, last,
    state, mix, seen, summer, sums, work,
    measured_raw, noise_raw, couples_raw, target_raw, jitter_raw, jitter_all,
    measured_row, noise_row, early_row, late_row, target_row,
    pred_out, pred_in, mine, members_in, stats_in,
    there_send, there_recv, back_send, back_recv, early_send, early_recv,
    a_send, a_recv, b_send, b_recv, r_send, r_recv, c_send, c_recv,
    look_sem, own_sem, small_sem, go_sem,
):
    me = lax.axis_index("mem")
    tile = lax.axis_index("pix")
    rows, cells = prior.shape
    members = rows // times
    total_members = members * parts
    width = cells // parts
    size = spans(width)
    first = [sum(size[:c]) for c in range(CHUNKS)]
    tail = size[-1]
    obs = target.shape[0]
    padded = target_row.shape[1]
    share = padded // tiles
    tile_blocks = cells // BLK
    look = seen.shape[2]
    looks = cells // look

    def small(i, source, dest):
        return pltpu.make_async_copy(source, dest, small_sem.at[i])

    loads = [
        small(0, measured, measured_raw),
        small(1, noise, noise_raw),
        small(2, couples, couples_raw),
        small(3, target, target_raw),
        small(4, jitter, jitter_raw),
    ]

    def look_copy(i):
        return pltpu.make_async_copy(
            prior.at[:, aligned(i, look)], seen.at[lax.rem(i, 2)], look_sem.at[lax.rem(i, 2)]
        )

    own = pltpu.make_async_copy(prior.at[:, aligned(me, width)], state.at[pl.ds(0, rows), :], own_sem)

    def there(k, c):
        column = pl.multiple_of((me ^ k) * width + first[c], LANES)
        return pltpu.make_async_remote_copy(
            src_ref=prior.at[:, pl.ds(column, size[c])],
            dst_ref=state.at[pl.ds(k * rows, rows), pl.ds(first[c], size[c])],
            send_sem=there_send,
            recv_sem=there_recv.at[c],
            device_id={"mem": me ^ k},
            device_id_type=MESH,
        )

    def back(k, c):
        column = pl.multiple_of(me * (width - tail) + first[c], LANES)
        return pltpu.make_async_remote_copy(
            src_ref=state.at[pl.ds(k * rows, rows), pl.ds(first[c], size[c])],
            dst_ref=out.at[:, pl.ds(column, size[c])],
            send_sem=back_send,
            recv_sem=back_recv,
            device_id={"mem": me ^ k},
            device_id_type=MESH,
        )

    def early(k):
        return pltpu.make_async_remote_copy(
            src_ref=last.at[pl.ds(k * rows, rows), :],
            dst_ref=rest.at[:, aligned(me, tail)],
            send_sem=early_send,
            recv_sem=early_recv,
            device_id={"mem": me ^ k},
            device_id_type=MESH,
        )

    def along(d):
        return lax.rem(tile + d, tiles)

    def send_a(d):
        return pltpu.make_async_remote_copy(
            src_ref=pred_out.at[along(d)],
            dst_ref=pred_in.at[tile],
            send_sem=a_send,
            recv_sem=a_recv,
            device_id={"pix": along(d)},
            device_id_type=MESH,
        )

    def send_b(k):
        return pltpu.make_async_remote_copy(
            src_ref=mine,
            dst_ref=members_in.at[me],
            send_sem=b_send,
            recv_sem=b_recv,
            device_id={"mem": me ^ k},
            device_id_type=MESH,
        )

    def relay(k):
        return pltpu.make_async_remote_copy(
            src_ref=members_in.at[me ^ k],
            dst_ref=members_in.at[me ^ k],
            send_sem=r_send,
            recv_sem=r_recv,
            device_id={"mem": me ^ 1},
            device_id_type=MESH,
        )

    def send_c(d):
        return pltpu.make_async_remote_copy(
            src_ref=stats_in.at[tile],
            dst_ref=stats_in.at[tile],
            send_sem=c_send,
            recv_sem=c_recv,
            device_id={"pix": along(d)},
            device_id_type=MESH,
        )

    def whole(region, send_sem, recv_sem):
        return pltpu.make_async_remote_copy(
            src_ref=region,
            dst_ref=region,
            send_sem=send_sem,
            recv_sem=recv_sem,
            device_id={"mem": me ^ 1},
            device_id_type=MESH,
        )

    partners = list(reversed(range(1, parts)))
    evens = partners[1::2]
    others = list(range(1, tiles))

    barrier = pltpu.get_barrier_semaphore()
    for k in partners:
        pl.semaphore_signal(barrier, inc=1, device_id={"mem": me ^ k}, device_id_type=MESH)
    look_copy(0).start()
    for load in loads:
        load.start()

    speaker = me == parts - 1
    root = jnp.logical_and(speaker, tile == tiles - 1)
    branch = jnp.logical_and(speaker, tile != tiles - 1)

    @pl.when(jnp.logical_not(root))
    def _():
        pl.semaphore_wait(barrier, len(partners))

    @pl.when(branch)
    def _():
        root_id = {"mem": me, "pix": tiles - 1}
        pl.semaphore_signal(barrier, inc=1, device_id=root_id, device_id_type=MESH)

    @pl.when(root)
    def _():
        pl.semaphore_wait(barrier, len(partners) + len(others))
        for d in others:
            pl.semaphore_signal(go_sem, inc=1, device_id={"pix": along(d)}, device_id_type=MESH)
        for k in partners:
            pl.semaphore_signal(go_sem, inc=1, device_id={"mem": me ^ k}, device_id_type=MESH)

    for k in partners:
        there(k, 0).start()
    own.start()

    summer[...] = (iota((look, LANES), 0) // BLK == iota((look, LANES), 1)).astype(BF16)

    def look_step(i, carry):
        @pl.when(i + 1 < looks)
        def _():
            look_copy(i + 1).start()

        look_copy(i).wait()
        sums[:, aligned(i, LANES)] = jnp.dot(
            seen[lax.rem(i, 2)], summer[...], preferred_element_type=F32
        )
        return carry

    lax.fori_loop(0, looks, look_step, 0)

    for load in loads:
        load.wait()
    measured_row[...] = jnp.zeros((1, padded), F32)
    noise_row[...] = jnp.ones((1, padded), F32)
    early_row[...] = jnp.zeros((1, padded), jnp.int32)
    late_row[...] = jnp.zeros((1, padded), jnp.int32)
    target_row[...] = jnp.full((1, padded), -1, jnp.int32)
    measured_row[:, :obs] = measured_raw[...].reshape(1, obs)
    noise_row[:, :obs] = noise_raw[...].reshape(1, obs)
    early_row[:, :obs] = couples_raw[0:1, :]
    late_row[:, :obs] = couples_raw[1:2, :]
    target_row[:, :obs] = target_raw[...].reshape(1, obs) - tile * tile_blocks
    jitter_all[...] = jnp.zeros((PASS_COUNT, total_members, padded), F32)
    jitter_all[:, :, :obs] = jitter_raw[...]

    def predict(i, carry):
        lanes = aligned(i, share)
        table = (target_row[:, lanes] == iota((tile_blocks, share), 0)).astype(F32)
        part = nn(sums[...], table)
        scene = iota((rows, share), 0) % times
        pair = (scene == late_row[:, lanes]).astype(F32) - (scene == early_row[:, lanes]).astype(F32)
        group = (iota((members, rows), 1) // times == iota((members, rows), 0)).astype(F32)
        pred_out[i] = nn(group, part * pair) / BLK
        return carry

    lax.fori_loop(0, tiles, predict, 0)

    @pl.when(jnp.logical_not(root))
    def _():
        pl.semaphore_wait(go_sem, 1)

    @pl.when(branch)
    def _():
        for k in partners:
            pl.semaphore_signal(go_sem, inc=1, device_id={"mem": me ^ k}, device_id_type=MESH)

    for d in others:
        send_a(d).start()
    pred_in[tile] = pred_out[tile]
    whole(pred_in.at[pl.ds(0, len(others))], a_send, a_recv).wait()
    total = pred_in[0]
    for d in others:
        total = total + pred_in[d]
    mine[...] = total
    members_in[me] = total
    for k in evens + [1]:
        send_b(k).start()
    for c in range(1, CHUNKS):
        for k in partners:
            there(k, c).start()
    whole(members_in.at[pl.ds(0, len(evens) + 1)], b_send, b_recv).wait()
    for k in evens:
        relay(k).start()
    whole(members_in.at[pl.ds(0, len(evens))], r_send, r_recv).wait()

    pred = jnp.concatenate([members_in[i] for i in range(parts)], axis=0)
    lanes = aligned(tile, share)
    here = (iota((1, share), 1) + tile * share < obs).astype(F32)
    mean = jnp.mean(pred, axis=0, keepdims=True)
    scale = math.sqrt(float(PASS_COUNT)) * noise_row[:, lanes]
    centred = (pred - mean) / scale * here
    gap = jnp.broadcast_to((measured_row[:, lanes] - mean) / scale * here, pred.shape)
    stats_in[tile, 0] = nt(centred, jnp.concatenate([centred, gap], axis=0))
    shakes = jnp.concatenate([jitter_all[i, :, lanes] for i in range(PASS_COUNT)], axis=0)
    stats_in[tile, 1] = nt(centred, shakes)
    for d in others:
        send_c(d).start()
    whole(stats_in.at[pl.ds(0, len(others))], c_send, c_recv).wait()
    total = stats_in[0]
    for d in others:
        total = total + stats_in[d]

    expand(solve(total, work), me, parts, times, mix)

    own.wait()
    step = math.gcd(256, *size)
    depth = parts * rows
    for c in range(CHUNKS):
        arrived = state.at[pl.ds(rows, depth - rows), pl.ds(first[c], size[c])]
        whole(arrived, there_send, there_recv.at[c]).wait_recv()

        def update(i, carry):
            columns = pl.ds(pl.multiple_of(first[c] + i * step, step), step)
            x = state[:, columns]
            both = jnp.dot(mix[...], x, preferred_element_type=F32)
            y = (x.astype(F32) + both[:depth] + both[depth:]).astype(BF16)
            if c < CHUNKS - 1:
                state[:, columns] = y
                column = me * (width - tail) + first[c] + i * step
                out[:, pl.ds(pl.multiple_of(column, step), step)] = y[:rows]
            else:
                last[:, aligned(i, step)] = y
                rest[:, pl.ds(pl.multiple_of(me * tail + i * step, step), step)] = y[:rows]
            return carry

        lax.fori_loop(0, size[c] // step, update, 0)
        if c < CHUNKS - 1:
            for k in partners:
                back(k, c).start()

    odd = lax.rem(me, 2) == 1

    @pl.when(odd)
    def _():
        for k in evens:
            early(k).start()

    whole(state.at[pl.ds(rows, depth - rows), :], there_send, back_recv).wait_send()
    moved = state.at[pl.ds(rows, depth - rows), pl.ds(0, width - tail)]
    whole(moved, back_send, back_recv).wait()

    @pl.when(odd)
    def _():
        whole(last.at[pl.ds(0, len(evens) * rows), :], early_send, early_recv).wait()


def finish_kernel(parts, before, last, out, send_sem, recv_sem, go_sem):
    me = lax.axis_index("mem")
    rows = out.shape[0]
    span = last.shape[1]
    partners = list(reversed(range(1, parts)))
    evens = partners[1::2]
    odds = partners[0::2]
    odd = lax.rem(me, 2) == 1
    even = jnp.logical_not(odd)
    barrier = pltpu.get_barrier_semaphore()

    def copy(k):
        return pltpu.make_async_remote_copy(
            src_ref=last.at[pl.ds(k * rows, rows), :],
            dst_ref=out.at[:, aligned(me, span)],
            send_sem=send_sem,
            recv_sem=recv_sem,
            device_id={"mem": me ^ k},
            device_id_type=MESH,
        )

    def signal(sem, k):
        pl.semaphore_signal(sem, inc=1, device_id={"mem": me ^ k}, device_id_type=MESH)

    def settle(count):
        region = last.at[pl.ds(0, count * rows), :]
        pltpu.make_async_remote_copy(
            src_ref=region,
            dst_ref=region,
            send_sem=send_sem,
            recv_sem=recv_sem,
            device_id={"mem": me ^ 1},
            device_id_type=MESH,
        ).wait()

    @pl.when(even)
    def _():
        for k in partners:
            signal(barrier, k)
        pl.semaphore_wait(barrier, len(evens))
        for k in evens:
            copy(k).start()
        pl.semaphore_wait(go_sem, len(odds))

    @pl.when(odd)
    def _():
        pl.semaphore_wait(barrier, len(odds))
        for k in odds:
            signal(go_sem, k)

    for k in odds:
        copy(k).start()

    @pl.when(odd)
    def _():
        settle(len(odds))

    @pl.when(even)
    def _():
        settle(len(partners))


def run(copies):
    for copy in copies:
        copy.start()
    for copy in copies:
        copy.wait()


def tail_piece(k, width, rest, out, sem):
    owner = lax.axis_index("mem") ^ k
    span = rest.shape[1] * width // out.shape[1]
    column = pl.multiple_of(owner * width + width - span, LANES)
    return pltpu.make_async_copy(
        rest.at[:, aligned(owner, span)], out.at[:, pl.ds(column, span)], sem.at[k]
    )


def write_most_kernel(parts, width, most, rest, out, sem, tail_sem):
    size = most.shape[1] // parts
    copies = [
        pltpu.make_async_copy(
            most.at[:, pl.ds(i * size, size)], out.at[:, pl.ds(i * width, size)], sem.at[i]
        )
        for i in range(parts)
    ]
    copies.append(tail_piece(0, width, rest, out, tail_sem))
    for copy in copies:
        copy.start()

    @pl.when(lax.rem(lax.axis_index("mem"), 2) == 1)
    def _():
        run([tail_piece(k, width, rest, out, tail_sem) for k in range(2, parts, 2)])

    for copy in copies:
        copy.wait()


def write_rest_kernel(parts, width, rest, before, out, sem):
    odd = lax.rem(lax.axis_index("mem"), 2) == 1

    @pl.when(odd)
    def _():
        run([tail_piece(k, width, rest, out, sem) for k in range(1, parts, 2)])

    @pl.when(jnp.logical_not(odd))
    def _():
        run([tail_piece(k, width, rest, out, sem) for k in range(1, parts)])


def body(prior, measured, noise, jitter, couples, target):
    parts = lax.axis_size("mem")
    tiles = lax.axis_size("pix")
    members, times, cells = prior.shape
    total_members = members * parts
    rows = members * times
    depth = rows * parts
    width = cells // parts
    obs = target.shape[0]
    unit = LANES * tiles
    padded = obs + (-obs) % unit
    share = padded // tiles
    look = LANES * BLK
    far = pl.BlockSpec(memory_space=pltpu.HBM)
    dma = pltpu.SemaphoreType.DMA
    scratch = [
        pltpu.VMEM((depth, width), BF16),
        pltpu.VMEM((2 * depth, depth), BF16),
        pltpu.VMEM((2, rows, look), BF16),
        pltpu.VMEM((look, LANES), BF16),
        pltpu.VMEM((rows, cells // BLK), F32),
        pltpu.VMEM((total_members, 2 * total_members), F32),
        pltpu.VMEM((obs,), F32),
        pltpu.VMEM((obs,), F32),
        pltpu.VMEM((2, obs), jnp.int32),
        pltpu.VMEM((obs,), jnp.int32),
        pltpu.VMEM((PASS_COUNT, total_members, obs), F32),
        pltpu.VMEM((PASS_COUNT, total_members, padded), F32),
        pltpu.VMEM((1, padded), F32),
        pltpu.VMEM((1, padded), F32),
        pltpu.VMEM((1, padded), jnp.int32),
        pltpu.VMEM((1, padded), jnp.int32),
        pltpu.VMEM((1, padded), jnp.int32),
        pltpu.VMEM((tiles, members, share), F32),
        pltpu.VMEM((tiles, members, share), F32),
        pltpu.VMEM((members, share), F32),
        pltpu.VMEM((parts, members, share), F32),
        pltpu.VMEM((tiles, 2, total_members, 2 * total_members), F32),
        dma,
        dma((CHUNKS,)),
        dma,
        dma,
        dma,
        dma,
        dma,
        dma,
        dma,
        dma,
        dma,
        dma,
        dma,
        dma,
        dma((2,)),
        dma,
        dma((5,)),
        pltpu.SemaphoreType.REGULAR,
    ]
    operands = (
        prior.reshape(rows, cells),
        measured,
        noise,
        jnp.swapaxes(jitter, 1, 2),
        couples,
        target,
    )
    span = spans(width)[-1]
    near = pl.BlockSpec(memory_space=pltpu.VMEM)
    most, rest, last = pl.pallas_call(
        functools.partial(smoother_kernel, parts, tiles, times),
        in_specs=[far] * 6,
        out_specs=[near] * 3,
        out_shape=[
            pltpu.VMEM((rows, parts * (width - span)), BF16),
            pltpu.VMEM((rows, parts * span), BF16),
            pltpu.VMEM((depth, span), BF16),
        ],
        scratch_shapes=scratch,
        compiler_params=pltpu.CompilerParams(
            collective_id=0, has_side_effects=True, vmem_limit_bytes=44 * 1024 * 1024
        ),
        name="smoother",
    )(*(pltpu.with_memory_space_constraint(a, pltpu.HBM) for a in operands))
    out = pl.pallas_call(
        functools.partial(write_most_kernel, parts, width),
        in_specs=[near, near],
        out_specs=far,
        out_shape=pltpu.HBM((rows, cells), BF16),
        scratch_shapes=[dma((parts,)), dma((parts,))],
        compiler_params=pltpu.CompilerParams(vmem_limit_bytes=4 * 1024 * 1024),
        name="write_most",
    )(most, rest)
    rest = pl.pallas_call(
        functools.partial(finish_kernel, parts),
        in_specs=[far, near],
        out_specs=near,
        out_shape=pltpu.VMEM((rows, parts * span), BF16),
        scratch_shapes=[dma, dma, pltpu.SemaphoreType.REGULAR],
        compiler_params=pltpu.CompilerParams(
            collective_id=1, has_side_effects=True, vmem_limit_bytes=8 * 1024 * 1024
        ),
        name="finish",
    )(pltpu.with_memory_space_constraint(out, pltpu.HBM), last)
    out = pl.pallas_call(
        functools.partial(write_rest_kernel, parts, width),
        in_specs=[near, far],
        out_specs=far,
        out_shape=pltpu.HBM((rows, cells), BF16),
        input_output_aliases={1: 0},
        scratch_shapes=[dma((parts,))],
        compiler_params=pltpu.CompilerParams(vmem_limit_bytes=4 * 1024 * 1024),
        name="write_rest",
    )(rest, out)
    return out.reshape(prior.shape)


def solution(mesh):
    return jax.shard_map(
        body,
        mesh=mesh,
        in_specs=(P("mem", None, "pix"), P(), P(), P(), P(), P()),
        out_specs=P("mem", None, "pix"),
        check_vma=False,
    )
```

```python
import functools
import math

import jax
import jax.numpy as jnp
from jax import lax
from jax.experimental import pallas as pl
from jax.experimental.pallas import tpu as pltpu
from jax.sharding import PartitionSpec as P

BLK = 64
PASS_COUNT = 2
LANES = 128
SHARES = (4, 4, 3, 5)
CHUNKS = len(SHARES)
F32 = jnp.float32
BF16 = jnp.bfloat16
HI = lax.Precision.HIGHEST
MESH = pl.DeviceIdType.MESH


def nn(a, b):
    return lax.dot_general(a, b, (((1,), (0,)), ((), ())), precision=HI, preferred_element_type=F32)


def tn(a, b):
    return nn(a.T, b)


def nt(a, b):
    return lax.dot_general(a, b, (((1,), (1,)), ((), ())), precision=HI, preferred_element_type=F32)


def iota(shape, axis):
    return lax.broadcasted_iota(jnp.int32, shape, axis)


def aligned(index, unit):
    return pl.ds(pl.multiple_of(index * unit, unit), unit)


def spans(width):
    return [width * part // sum(SHARES) for part in SHARES]


def gauss_jordan(matrix, right, work):
    n = matrix.shape[0]
    work[...] = jnp.concatenate([matrix, right], axis=1)
    row_id = iota((n, 1), 0)
    lane_id = iota((n, 2 * n), 1)

    def step(k, carry):
        table = work[...]
        row = work[pl.ds(k, 1), :]
        here = lane_id == k
        factor = jnp.sum(jnp.where(here, table, 0.0), axis=1, keepdims=True)
        pivot = row / jnp.sum(jnp.where(here[:1], row, 0.0), axis=1, keepdims=True)
        work[...] = jnp.where(row_id == k, pivot, table - factor * pivot)
        return carry

    lax.fori_loop(0, n, step, 0)
    return work[:, n:]


def solve(total, work):
    n = total[0].shape[0]
    s, g = total[0][:, :n], total[0][:, n:]
    h1, h2 = total[1][:, :n], total[1][:, n:]
    eye = (iota((n, n), 0) == iota((n, n), 1)).astype(F32)
    m1 = gauss_jordan(eye + s / (n - 1), (g + h1 - s) / (n - 1), work).astype(BF16).astype(F32)
    m1_mean = jnp.mean(m1, axis=1, keepdims=True)
    step = eye + m1 - m1_mean
    s2 = tn(step, nn(s, step))
    g2 = tn(step, g - nn(s, jnp.broadcast_to(m1_mean, (n, n))))
    h22 = tn(step, h2)
    m2 = gauss_jordan(eye + s2 / (n - 1), (g2 + h22 - s2) / (n - 1), work).astype(BF16).astype(F32)
    m2c = m2 - jnp.mean(m2, axis=0, keepdims=True)
    w = m1 + m2 + nn(m1, m2c)
    return w - jnp.mean(w, axis=0, keepdims=True)


def expand(w, me, parts, times, mix):
    n = w.shape[0]
    members = n // parts
    rows = members * times
    depth = rows * parts
    spot = iota((n, n), 0)
    source = ((spot // members) ^ me) * members + spot % members
    order = (iota((n, n), 1) == source).astype(F32)
    wt = nt(nn(order, w.T), order)
    hi = wt.astype(BF16)
    lo = (wt - hi.astype(F32)).astype(BF16)
    spread = (iota((n, depth), 1) // times == iota((n, depth), 0)).astype(BF16)
    tall = (iota((rows, members), 0) // times == iota((rows, members), 1)).astype(BF16)
    same = iota((rows, depth), 0) % times == iota((rows, depth), 1) % times
    for piece, first in ((hi, 0), (lo, depth)):
        wide = jnp.dot(piece, spread, preferred_element_type=F32).astype(BF16)
        for part in range(parts):
            block = jnp.dot(
                tall, wide[part * members : (part + 1) * members, :], preferred_element_type=F32
            )
            start = first + part * rows
            mix[start : start + rows, :] = jnp.where(same, block, 0.0).astype(BF16)


def smoother_kernel(
    parts, tiles, times,
    prior, measured, noise, jitter, couples, target, out, rest, last,
    state, mix, seen, summer, sums, work,
    measured_raw, noise_raw, couples_raw, target_raw, jitter_raw, jitter_all,
    measured_row, noise_row, early_row, late_row, target_row,
    pred_out, pred_in, mine, members_in, stats_in,
    there_send, there_recv, back_send, back_recv, early_send, early_recv,
    a_send, a_recv, b_send, b_recv, r_send, r_recv, c_send, c_recv,
    look_sem, own_sem, small_sem, go_sem,
):
    me = lax.axis_index("mem")
    tile = lax.axis_index("pix")
    rows, cells = prior.shape
    members = rows // times
    total_members = members * parts
    width = cells // parts
    size = spans(width)
    first = [sum(size[:c]) for c in range(CHUNKS)]
    tail = size[-1]
    obs = target.shape[0]
    padded = target_row.shape[1]
    share = padded // tiles
    tile_blocks = cells // BLK
    look = seen.shape[2]
    looks = cells // look

    def small(i, source, dest):
        return pltpu.make_async_copy(source, dest, small_sem.at[i])

    loads = [
        small(0, measured, measured_raw),
        small(1, noise, noise_raw),
        small(2, couples, couples_raw),
        small(3, target, target_raw),
        small(4, jitter, jitter_raw),
    ]

    def look_copy(i):
        return pltpu.make_async_copy(
            prior.at[:, aligned(i, look)], seen.at[lax.rem(i, 2)], look_sem.at[lax.rem(i, 2)]
        )

    own = pltpu.make_async_copy(prior.at[:, aligned(me, width)], state.at[pl.ds(0, rows), :], own_sem)

    def there(k, c):
        column = pl.multiple_of((me ^ k) * width + first[c], LANES)
        return pltpu.make_async_remote_copy(
            src_ref=prior.at[:, pl.ds(column, size[c])],
            dst_ref=state.at[pl.ds(k * rows, rows), pl.ds(first[c], size[c])],
            send_sem=there_send,
            recv_sem=there_recv.at[c],
            device_id={"mem": me ^ k},
            device_id_type=MESH,
        )

    def back(k, c):
        column = pl.multiple_of(me * (width - tail) + first[c], LANES)
        return pltpu.make_async_remote_copy(
            src_ref=state.at[pl.ds(k * rows, rows), pl.ds(first[c], size[c])],
            dst_ref=out.at[:, pl.ds(column, size[c])],
            send_sem=back_send,
            recv_sem=back_recv,
            device_id={"mem": me ^ k},
            device_id_type=MESH,
        )

    def early(k):
        return pltpu.make_async_remote_copy(
            src_ref=last.at[pl.ds(k * rows, rows), :],
            dst_ref=rest.at[:, aligned(me, tail)],
            send_sem=early_send,
            recv_sem=early_recv,
            device_id={"mem": me ^ k},
            device_id_type=MESH,
        )

    def along(d):
        return lax.rem(tile + d, tiles)

    def send_a(d):
        return pltpu.make_async_remote_copy(
            src_ref=pred_out.at[along(d)],
            dst_ref=pred_in.at[tile],
            send_sem=a_send,
            recv_sem=a_recv,
            device_id={"pix": along(d)},
            device_id_type=MESH,
        )

    def send_b(k):
        return pltpu.make_async_remote_copy(
            src_ref=mine,
            dst_ref=members_in.at[me],
            send_sem=b_send,
            recv_sem=b_recv,
            device_id={"mem": me ^ k},
            device_id_type=MESH,
        )

    def relay(k):
        return pltpu.make_async_remote_copy(
            src_ref=members_in.at[me ^ k],
            dst_ref=members_in.at[me ^ k],
            send_sem=r_send,
            recv_sem=r_recv,
            device_id={"mem": me ^ 1},
            device_id_type=MESH,
        )

    def send_c(d):
        return pltpu.make_async_remote_copy(
            src_ref=stats_in.at[tile],
            dst_ref=stats_in.at[tile],
            send_sem=c_send,
            recv_sem=c_recv,
            device_id={"pix": along(d)},
            device_id_type=MESH,
        )

    def whole(region, send_sem, recv_sem):
        return pltpu.make_async_remote_copy(
            src_ref=region,
            dst_ref=region,
            send_sem=send_sem,
            recv_sem=recv_sem,
            device_id={"mem": me ^ 1},
            device_id_type=MESH,
        )

    partners = list(range(1, parts))
    evens = partners[1::2]
    others = list(range(1, tiles))

    barrier = pltpu.get_barrier_semaphore()
    for k in partners:
        pl.semaphore_signal(barrier, inc=1, device_id={"mem": me ^ k}, device_id_type=MESH)
    look_copy(0).start()
    for load in loads:
        load.start()

    speaker = me == parts - 1
    root = jnp.logical_and(speaker, tile == tiles - 1)
    branch = jnp.logical_and(speaker, tile != tiles - 1)

    @pl.when(jnp.logical_not(root))
    def _():
        pl.semaphore_wait(barrier, len(partners))

    @pl.when(branch)
    def _():
        root_id = {"mem": me, "pix": tiles - 1}
        pl.semaphore_signal(barrier, inc=1, device_id=root_id, device_id_type=MESH)

    @pl.when(root)
    def _():
        pl.semaphore_wait(barrier, len(partners) + len(others))
        for d in others:
            pl.semaphore_signal(go_sem, inc=1, device_id={"pix": along(d)}, device_id_type=MESH)
        for k in partners:
            pl.semaphore_signal(go_sem, inc=1, device_id={"mem": me ^ k}, device_id_type=MESH)

    for k in partners:
        there(k, 0).start()
    own.start()

    summer[...] = (iota((look, LANES), 0) // BLK == iota((look, LANES), 1)).astype(BF16)

    def look_step(i, carry):
        @pl.when(i + 1 < looks)
        def _():
            look_copy(i + 1).start()

        look_copy(i).wait()
        sums[:, aligned(i, LANES)] = jnp.dot(
            seen[lax.rem(i, 2)], summer[...], preferred_element_type=F32
        )
        return carry

    lax.fori_loop(0, looks, look_step, 0)

    for load in loads:
        load.wait()
    measured_row[...] = jnp.zeros((1, padded), F32)
    noise_row[...] = jnp.ones((1, padded), F32)
    early_row[...] = jnp.zeros((1, padded), jnp.int32)
    late_row[...] = jnp.zeros((1, padded), jnp.int32)
    target_row[...] = jnp.full((1, padded), -1, jnp.int32)
    measured_row[:, :obs] = measured_raw[...].reshape(1, obs)
    noise_row[:, :obs] = noise_raw[...].reshape(1, obs)
    early_row[:, :obs] = couples_raw[0:1, :]
    late_row[:, :obs] = couples_raw[1:2, :]
    target_row[:, :obs] = target_raw[...].reshape(1, obs) - tile * tile_blocks
    jitter_all[...] = jnp.zeros((PASS_COUNT, total_members, padded), F32)
    jitter_all[:, :, :obs] = jitter_raw[...]

    def predict(i, carry):
        lanes = aligned(i, share)
        table = (target_row[:, lanes] == iota((tile_blocks, share), 0)).astype(F32)
        part = nn(sums[...], table)
        scene = iota((rows, share), 0) % times
        pair = (scene == late_row[:, lanes]).astype(F32) - (scene == early_row[:, lanes]).astype(F32)
        group = (iota((members, rows), 1) // times == iota((members, rows), 0)).astype(F32)
        pred_out[i] = nn(group, part * pair) / BLK
        return carry

    lax.fori_loop(0, tiles, predict, 0)

    @pl.when(jnp.logical_not(root))
    def _():
        pl.semaphore_wait(go_sem, 1)

    @pl.when(branch)
    def _():
        for k in partners:
            pl.semaphore_signal(go_sem, inc=1, device_id={"mem": me ^ k}, device_id_type=MESH)

    for d in others:
        send_a(d).start()
    pred_in[tile] = pred_out[tile]
    whole(pred_in.at[pl.ds(0, len(others))], a_send, a_recv).wait()
    total = pred_in[0]
    for d in others:
        total = total + pred_in[d]
    mine[...] = total
    members_in[me] = total
    for k in evens + [1]:
        send_b(k).start()
    for c in range(1, CHUNKS):
        for k in partners:
            there(k, c).start()
    whole(members_in.at[pl.ds(0, len(evens) + 1)], b_send, b_recv).wait()
    for k in evens:
        relay(k).start()
    whole(members_in.at[pl.ds(0, len(evens))], r_send, r_recv).wait()

    pred = jnp.concatenate([members_in[i] for i in range(parts)], axis=0)
    lanes = aligned(tile, share)
    here = (iota((1, share), 1) + tile * share < obs).astype(F32)
    mean = jnp.mean(pred, axis=0, keepdims=True)
    scale = math.sqrt(float(PASS_COUNT)) * noise_row[:, lanes]
    centred = (pred - mean) / scale * here
    gap = jnp.broadcast_to((measured_row[:, lanes] - mean) / scale * here, pred.shape)
    stats_in[tile, 0] = nt(centred, jnp.concatenate([centred, gap], axis=0))
    shakes = jnp.concatenate([jitter_all[i, :, lanes] for i in range(PASS_COUNT)], axis=0)
    stats_in[tile, 1] = nt(centred, shakes)
    for d in others:
        send_c(d).start()
    whole(stats_in.at[pl.ds(0, len(others))], c_send, c_recv).wait()
    total = stats_in[0]
    for d in others:
        total = total + stats_in[d]

    expand(solve(total, work), me, parts, times, mix)

    own.wait()
    step = math.gcd(256, *size)
    depth = parts * rows
    for c in range(CHUNKS):
        arrived = state.at[pl.ds(rows, depth - rows), pl.ds(first[c], size[c])]
        whole(arrived, there_send, there_recv.at[c]).wait_recv()

        def update(i, carry):
            columns = pl.ds(pl.multiple_of(first[c] + i * step, step), step)
            x = state[:, columns]
            both = jnp.dot(mix[...], x, preferred_element_type=F32)
            y = (x.astype(F32) + both[:depth] + both[depth:]).astype(BF16)
            if c < CHUNKS - 1:
                state[:, columns] = y
                column = me * (width - tail) + first[c] + i * step
                out[:, pl.ds(pl.multiple_of(column, step), step)] = y[:rows]
            else:
                last[:, aligned(i, step)] = y
                rest[:, pl.ds(pl.multiple_of(me * tail + i * step, step), step)] = y[:rows]
            return carry

        lax.fori_loop(0, size[c] // step, update, 0)
        if c < CHUNKS - 1:
            for k in partners:
                back(k, c).start()

    odd = lax.rem(me, 2) == 1

    @pl.when(odd)
    def _():
        for k in evens:
            early(k).start()

    whole(state.at[pl.ds(rows, depth - rows), :], there_send, back_recv).wait_send()
    moved = state.at[pl.ds(rows, depth - rows), pl.ds(0, width - tail)]
    whole(moved, back_send, back_recv).wait()

    @pl.when(odd)
    def _():
        whole(last.at[pl.ds(0, len(evens) * rows), :], early_send, early_recv).wait()


def finish_kernel(parts, before, last, out, send_sem, recv_sem, go_sem):
    me = lax.axis_index("mem")
    rows = out.shape[0]
    span = last.shape[1]
    partners = list(reversed(range(1, parts)))
    evens = partners[1::2]
    odds = partners[0::2]
    odd = lax.rem(me, 2) == 1
    even = jnp.logical_not(odd)
    barrier = pltpu.get_barrier_semaphore()

    def copy(k):
        return pltpu.make_async_remote_copy(
            src_ref=last.at[pl.ds(k * rows, rows), :],
            dst_ref=out.at[:, aligned(me, span)],
            send_sem=send_sem,
            recv_sem=recv_sem,
            device_id={"mem": me ^ k},
            device_id_type=MESH,
        )

    def signal(sem, k):
        pl.semaphore_signal(sem, inc=1, device_id={"mem": me ^ k}, device_id_type=MESH)

    def settle(count):
        region = last.at[pl.ds(0, count * rows), :]
        pltpu.make_async_remote_copy(
            src_ref=region,
            dst_ref=region,
            send_sem=send_sem,
            recv_sem=recv_sem,
            device_id={"mem": me ^ 1},
            device_id_type=MESH,
        ).wait()

    @pl.when(even)
    def _():
        for k in partners:
            signal(barrier, k)
        pl.semaphore_wait(barrier, len(evens))
        for k in evens:
            copy(k).start()
        pl.semaphore_wait(go_sem, len(odds))

    @pl.when(odd)
    def _():
        pl.semaphore_wait(barrier, len(odds))
        for k in odds:
            signal(go_sem, k)

    for k in odds:
        copy(k).start()

    @pl.when(odd)
    def _():
        settle(len(odds))

    @pl.when(even)
    def _():
        settle(len(partners))


def run(copies):
    for copy in copies:
        copy.start()
    for copy in copies:
        copy.wait()


def tail_piece(k, width, rest, out, sem):
    owner = lax.axis_index("mem") ^ k
    span = rest.shape[1] * width // out.shape[1]
    column = pl.multiple_of(owner * width + width - span, LANES)
    return pltpu.make_async_copy(
        rest.at[:, aligned(owner, span)], out.at[:, pl.ds(column, span)], sem.at[k]
    )


def write_most_kernel(parts, width, most, rest, out, sem, tail_sem):
    size = most.shape[1] // parts
    copies = [
        pltpu.make_async_copy(
            most.at[:, pl.ds(i * size, size)], out.at[:, pl.ds(i * width, size)], sem.at[i]
        )
        for i in range(parts)
    ]
    copies.append(tail_piece(0, width, rest, out, tail_sem))
    for copy in copies:
        copy.start()

    @pl.when(lax.rem(lax.axis_index("mem"), 2) == 1)
    def _():
        run([tail_piece(k, width, rest, out, tail_sem) for k in range(2, parts, 2)])

    for copy in copies:
        copy.wait()


def write_rest_kernel(parts, width, rest, before, out, sem):
    odd = lax.rem(lax.axis_index("mem"), 2) == 1

    @pl.when(odd)
    def _():
        run([tail_piece(k, width, rest, out, sem) for k in range(1, parts, 2)])

    @pl.when(jnp.logical_not(odd))
    def _():
        run([tail_piece(k, width, rest, out, sem) for k in range(1, parts)])


def body(prior, measured, noise, jitter, couples, target):
    parts = lax.axis_size("mem")
    tiles = lax.axis_size("pix")
    members, times, cells = prior.shape
    total_members = members * parts
    rows = members * times
    depth = rows * parts
    width = cells // parts
    obs = target.shape[0]
    unit = LANES * tiles
    padded = obs + (-obs) % unit
    share = padded // tiles
    look = LANES * BLK
    far = pl.BlockSpec(memory_space=pltpu.HBM)
    dma = pltpu.SemaphoreType.DMA
    scratch = [
        pltpu.VMEM((depth, width), BF16),
        pltpu.VMEM((2 * depth, depth), BF16),
        pltpu.VMEM((2, rows, look), BF16),
        pltpu.VMEM((look, LANES), BF16),
        pltpu.VMEM((rows, cells // BLK), F32),
        pltpu.VMEM((total_members, 2 * total_members), F32),
        pltpu.VMEM((obs,), F32),
        pltpu.VMEM((obs,), F32),
        pltpu.VMEM((2, obs), jnp.int32),
        pltpu.VMEM((obs,), jnp.int32),
        pltpu.VMEM((PASS_COUNT, total_members, obs), F32),
        pltpu.VMEM((PASS_COUNT, total_members, padded), F32),
        pltpu.VMEM((1, padded), F32),
        pltpu.VMEM((1, padded), F32),
        pltpu.VMEM((1, padded), jnp.int32),
        pltpu.VMEM((1, padded), jnp.int32),
        pltpu.VMEM((1, padded), jnp.int32),
        pltpu.VMEM((tiles, members, share), F32),
        pltpu.VMEM((tiles, members, share), F32),
        pltpu.VMEM((members, share), F32),
        pltpu.VMEM((parts, members, share), F32),
        pltpu.VMEM((tiles, 2, total_members, 2 * total_members), F32),
        dma,
        dma((CHUNKS,)),
        dma,
        dma,
        dma,
        dma,
        dma,
        dma,
        dma,
        dma,
        dma,
        dma,
        dma,
        dma,
        dma((2,)),
        dma,
        dma((5,)),
        pltpu.SemaphoreType.REGULAR,
    ]
    operands = (
        prior.reshape(rows, cells),
        measured,
        noise,
        jnp.swapaxes(jitter, 1, 2),
        couples,
        target,
    )
    span = spans(width)[-1]
    near = pl.BlockSpec(memory_space=pltpu.VMEM)
    most, rest, last = pl.pallas_call(
        functools.partial(smoother_kernel, parts, tiles, times),
        in_specs=[far] * 6,
        out_specs=[near] * 3,
        out_shape=[
            pltpu.VMEM((rows, parts * (width - span)), BF16),
            pltpu.VMEM((rows, parts * span), BF16),
            pltpu.VMEM((depth, span), BF16),
        ],
        scratch_shapes=scratch,
        compiler_params=pltpu.CompilerParams(
            collective_id=0, has_side_effects=True, vmem_limit_bytes=44 * 1024 * 1024
        ),
        name="smoother",
    )(*(pltpu.with_memory_space_constraint(a, pltpu.HBM) for a in operands))
    out = pl.pallas_call(
        functools.partial(write_most_kernel, parts, width),
        in_specs=[near, near],
        out_specs=far,
        out_shape=pltpu.HBM((rows, cells), BF16),
        scratch_shapes=[dma((parts,)), dma((parts,))],
        compiler_params=pltpu.CompilerParams(vmem_limit_bytes=4 * 1024 * 1024),
        name="write_most",
    )(most, rest)
    rest = pl.pallas_call(
        functools.partial(finish_kernel, parts),
        in_specs=[far, near],
        out_specs=near,
        out_shape=pltpu.VMEM((rows, parts * span), BF16),
        scratch_shapes=[dma, dma, pltpu.SemaphoreType.REGULAR],
        compiler_params=pltpu.CompilerParams(
            collective_id=1, has_side_effects=True, vmem_limit_bytes=8 * 1024 * 1024
        ),
        name="finish",
    )(pltpu.with_memory_space_constraint(out, pltpu.HBM), last)
    out = pl.pallas_call(
        functools.partial(write_rest_kernel, parts, width),
        in_specs=[near, far],
        out_specs=far,
        out_shape=pltpu.HBM((rows, cells), BF16),
        input_output_aliases={1: 0},
        scratch_shapes=[dma((parts,))],
        compiler_params=pltpu.CompilerParams(vmem_limit_bytes=4 * 1024 * 1024),
        name="write_rest",
    )(rest, out)
    return out.reshape(prior.shape)


def solution(mesh):
    return jax.shard_map(
        body,
        mesh=mesh,
        in_specs=(P("mem", None, "pix"), P(), P(), P(), P(), P()),
        out_specs=P("mem", None, "pix"),
        check_vma=False,
    )
```

```python
import functools
import math

import jax
import jax.numpy as jnp
from jax import lax
from jax.experimental import pallas as pl
from jax.experimental.pallas import tpu as pltpu
from jax.sharding import PartitionSpec as P

BLK = 64
PASS_COUNT = 2
LANES = 128
SHARES = (4, 4, 3, 5)
CHUNKS = len(SHARES)
F32 = jnp.float32
BF16 = jnp.bfloat16
HI = lax.Precision.HIGHEST
MESH = pl.DeviceIdType.MESH


def nn(a, b):
    return lax.dot_general(a, b, (((1,), (0,)), ((), ())), precision=HI, preferred_element_type=F32)


def tn(a, b):
    return nn(a.T, b)


def nt(a, b):
    return lax.dot_general(a, b, (((1,), (1,)), ((), ())), precision=HI, preferred_element_type=F32)


def iota(shape, axis):
    return lax.broadcasted_iota(jnp.int32, shape, axis)


def aligned(index, unit):
    return pl.ds(pl.multiple_of(index * unit, unit), unit)


def spans(width):
    return [width * part // sum(SHARES) for part in SHARES]


def gauss_jordan(matrix, right, work):
    n = matrix.shape[0]
    work[...] = jnp.concatenate([matrix, right], axis=1)
    row_id = iota((n, 1), 0)
    lane_id = iota((n, 2 * n), 1)

    def step(k, carry):
        table = work[...]
        row = work[pl.ds(k, 1), :]
        here = lane_id == k
        factor = jnp.sum(jnp.where(here, table, 0.0), axis=1, keepdims=True)
        pivot = row / jnp.sum(jnp.where(here[:1], row, 0.0), axis=1, keepdims=True)
        work[...] = jnp.where(row_id == k, pivot, table - factor * pivot)
        return carry

    lax.fori_loop(0, n, step, 0)
    return work[:, n:]


def solve(total, work):
    n = total[0].shape[0]
    s, g = total[0][:, :n], total[0][:, n:]
    h1, h2 = total[1][:, :n], total[1][:, n:]
    eye = (iota((n, n), 0) == iota((n, n), 1)).astype(F32)
    m1 = gauss_jordan(eye + s / (n - 1), (g + h1 - s) / (n - 1), work).astype(BF16).astype(F32)
    m1_mean = jnp.mean(m1, axis=1, keepdims=True)
    step = eye + m1 - m1_mean
    s2 = tn(step, nn(s, step))
    g2 = tn(step, g - nn(s, jnp.broadcast_to(m1_mean, (n, n))))
    h22 = tn(step, h2)
    m2 = gauss_jordan(eye + s2 / (n - 1), (g2 + h22 - s2) / (n - 1), work).astype(BF16).astype(F32)
    m2c = m2 - jnp.mean(m2, axis=0, keepdims=True)
    w = m1 + m2 + nn(m1, m2c)
    return w - jnp.mean(w, axis=0, keepdims=True)


def expand(w, me, parts, times, mix):
    n = w.shape[0]
    members = n // parts
    rows = members * times
    depth = rows * parts
    spot = iota((n, n), 0)
    source = ((spot // members) ^ me) * members + spot % members
    order = (iota((n, n), 1) == source).astype(F32)
    wt = nt(nn(order, w.T), order)
    hi = wt.astype(BF16)
    lo = (wt - hi.astype(F32)).astype(BF16)
    spread = (iota((n, depth), 1) // times == iota((n, depth), 0)).astype(BF16)
    tall = (iota((rows, members), 0) // times == iota((rows, members), 1)).astype(BF16)
    same = iota((rows, depth), 0) % times == iota((rows, depth), 1) % times
    for piece, first in ((hi, 0), (lo, depth)):
        wide = jnp.dot(piece, spread, preferred_element_type=F32).astype(BF16)
        for part in range(parts):
            block = jnp.dot(
                tall, wide[part * members : (part + 1) * members, :], preferred_element_type=F32
            )
            start = first + part * rows
            mix[start : start + rows, :] = jnp.where(same, block, 0.0).astype(BF16)


def smoother_kernel(
    parts, tiles, times,
    prior, measured, noise, jitter, couples, target, out, rest, last,
    state, mix, seen, summer, sums, work,
    measured_raw, noise_raw, couples_raw, target_raw, jitter_raw, jitter_all,
    measured_row, noise_row, early_row, late_row, target_row,
    pred_out, pred_in, mine, members_in, stats_in,
    there_send, there_recv, back_send, back_recv, early_send, early_recv,
    a_send, a_recv, b_send, b_recv, r_send, r_recv, c_send, c_recv,
    look_sem, own_sem, small_sem, go_sem,
):
    me = lax.axis_index("mem")
    tile = lax.axis_index("pix")
    rows, cells = prior.shape
    members = rows // times
    total_members = members * parts
    width = cells // parts
    size = spans(width)
    first = [sum(size[:c]) for c in range(CHUNKS)]
    tail = size[-1]
    obs = target.shape[0]
    padded = target_row.shape[1]
    share = padded // tiles
    tile_blocks = cells // BLK
    look = seen.shape[2]
    looks = cells // look

    def small(i, source, dest):
        return pltpu.make_async_copy(source, dest, small_sem.at[i])

    loads = [
        small(0, measured, measured_raw),
        small(1, noise, noise_raw),
        small(2, couples, couples_raw),
        small(3, target, target_raw),
        small(4, jitter, jitter_raw),
    ]

    def look_copy(i):
        return pltpu.make_async_copy(
            prior.at[:, aligned(i, look)], seen.at[lax.rem(i, 2)], look_sem.at[lax.rem(i, 2)]
        )

    own = pltpu.make_async_copy(prior.at[:, aligned(me, width)], state.at[pl.ds(0, rows), :], own_sem)

    def there(k, c):
        column = pl.multiple_of((me ^ k) * width + first[c], LANES)
        return pltpu.make_async_remote_copy(
            src_ref=prior.at[:, pl.ds(column, size[c])],
            dst_ref=state.at[pl.ds(k * rows, rows), pl.ds(first[c], size[c])],
            send_sem=there_send,
            recv_sem=there_recv.at[c],
            device_id={"mem": me ^ k},
            device_id_type=MESH,
        )

    def back(k, c):
        column = pl.multiple_of(me * (width - tail) + first[c], LANES)
        return pltpu.make_async_remote_copy(
            src_ref=state.at[pl.ds(k * rows, rows), pl.ds(first[c], size[c])],
            dst_ref=out.at[:, pl.ds(column, size[c])],
            send_sem=back_send,
            recv_sem=back_recv,
            device_id={"mem": me ^ k},
            device_id_type=MESH,
        )

    def early(k):
        return pltpu.make_async_remote_copy(
            src_ref=last.at[pl.ds(k * rows, rows), :],
            dst_ref=rest.at[:, aligned(me, tail)],
            send_sem=early_send,
            recv_sem=early_recv,
            device_id={"mem": me ^ k},
            device_id_type=MESH,
        )

    def along(d):
        return lax.rem(tile + d, tiles)

    def send_a(d):
        return pltpu.make_async_remote_copy(
            src_ref=pred_out.at[along(d)],
            dst_ref=pred_in.at[tile],
            send_sem=a_send,
            recv_sem=a_recv,
            device_id={"pix": along(d)},
            device_id_type=MESH,
        )

    def send_b(k):
        return pltpu.make_async_remote_copy(
            src_ref=mine,
            dst_ref=members_in.at[me],
            send_sem=b_send,
            recv_sem=b_recv,
            device_id={"mem": me ^ k},
            device_id_type=MESH,
        )

    def relay(k):
        return pltpu.make_async_remote_copy(
            src_ref=members_in.at[me ^ k],
            dst_ref=members_in.at[me ^ k],
            send_sem=r_send,
            recv_sem=r_recv,
            device_id={"mem": me ^ 1},
            device_id_type=MESH,
        )

    def send_c(d):
        return pltpu.make_async_remote_copy(
            src_ref=stats_in.at[tile],
            dst_ref=stats_in.at[tile],
            send_sem=c_send,
            recv_sem=c_recv,
            device_id={"pix": along(d)},
            device_id_type=MESH,
        )

    def whole(region, send_sem, recv_sem):
        return pltpu.make_async_remote_copy(
            src_ref=region,
            dst_ref=region,
            send_sem=send_sem,
            recv_sem=recv_sem,
            device_id={"mem": me ^ 1},
            device_id_type=MESH,
        )

    partners = list(range(1, parts))
    evens = partners[1::2]
    others = list(range(1, tiles))

    barrier = pltpu.get_barrier_semaphore()
    for k in partners:
        pl.semaphore_signal(barrier, inc=1, device_id={"mem": me ^ k}, device_id_type=MESH)

    speaker = me == parts - 1
    root = jnp.logical_and(speaker, tile == tiles - 1)
    branch = jnp.logical_and(speaker, tile != tiles - 1)

    @pl.when(jnp.logical_not(root))
    def _():
        pl.semaphore_wait(barrier, len(partners))

    @pl.when(branch)
    def _():
        root_id = {"mem": me, "pix": tiles - 1}
        pl.semaphore_signal(barrier, inc=1, device_id=root_id, device_id_type=MESH)

    @pl.when(root)
    def _():
        pl.semaphore_wait(barrier, len(partners) + len(others))
        for d in others:
            pl.semaphore_signal(go_sem, inc=1, device_id={"pix": along(d)}, device_id_type=MESH)
        for k in partners:
            pl.semaphore_signal(go_sem, inc=1, device_id={"mem": me ^ k}, device_id_type=MESH)

    for k in partners:
        there(k, 0).start()
    look_copy(0).start()
    for load in loads:
        load.start()
    own.start()

    summer[...] = (iota((look, LANES), 0) // BLK == iota((look, LANES), 1)).astype(BF16)

    def look_step(i, carry):
        @pl.when(i + 1 < looks)
        def _():
            look_copy(i + 1).start()

        look_copy(i).wait()
        sums[:, aligned(i, LANES)] = jnp.dot(
            seen[lax.rem(i, 2)], summer[...], preferred_element_type=F32
        )
        return carry

    lax.fori_loop(0, looks, look_step, 0)

    for load in loads:
        load.wait()
    measured_row[...] = jnp.zeros((1, padded), F32)
    noise_row[...] = jnp.ones((1, padded), F32)
    early_row[...] = jnp.zeros((1, padded), jnp.int32)
    late_row[...] = jnp.zeros((1, padded), jnp.int32)
    target_row[...] = jnp.full((1, padded), -1, jnp.int32)
    measured_row[:, :obs] = measured_raw[...].reshape(1, obs)
    noise_row[:, :obs] = noise_raw[...].reshape(1, obs)
    early_row[:, :obs] = couples_raw[0:1, :]
    late_row[:, :obs] = couples_raw[1:2, :]
    target_row[:, :obs] = target_raw[...].reshape(1, obs) - tile * tile_blocks
    jitter_all[...] = jnp.zeros((PASS_COUNT, total_members, padded), F32)
    jitter_all[:, :, :obs] = jitter_raw[...]

    def predict(i, carry):
        lanes = aligned(i, share)
        table = (target_row[:, lanes] == iota((tile_blocks, share), 0)).astype(F32)
        part = nn(sums[...], table)
        scene = iota((rows, share), 0) % times
        pair = (scene == late_row[:, lanes]).astype(F32) - (scene == early_row[:, lanes]).astype(F32)
        group = (iota((members, rows), 1) // times == iota((members, rows), 0)).astype(F32)
        pred_out[i] = nn(group, part * pair) / BLK
        return carry

    lax.fori_loop(0, tiles, predict, 0)

    @pl.when(jnp.logical_not(root))
    def _():
        pl.semaphore_wait(go_sem, 1)

    @pl.when(branch)
    def _():
        for k in partners:
            pl.semaphore_signal(go_sem, inc=1, device_id={"mem": me ^ k}, device_id_type=MESH)

    for d in others:
        send_a(d).start()
    pred_in[tile] = pred_out[tile]
    whole(pred_in.at[pl.ds(0, len(others))], a_send, a_recv).wait()
    total = pred_in[0]
    for d in others:
        total = total + pred_in[d]
    mine[...] = total
    members_in[me] = total
    for k in evens + [1]:
        send_b(k).start()
    for c in range(1, CHUNKS):
        for k in partners:
            there(k, c).start()
    whole(members_in.at[pl.ds(0, len(evens) + 1)], b_send, b_recv).wait()
    for k in evens:
        relay(k).start()
    whole(members_in.at[pl.ds(0, len(evens))], r_send, r_recv).wait()

    pred = jnp.concatenate([members_in[i] for i in range(parts)], axis=0)
    lanes = aligned(tile, share)
    here = (iota((1, share), 1) + tile * share < obs).astype(F32)
    mean = jnp.mean(pred, axis=0, keepdims=True)
    scale = math.sqrt(float(PASS_COUNT)) * noise_row[:, lanes]
    centred = (pred - mean) / scale * here
    gap = jnp.broadcast_to((measured_row[:, lanes] - mean) / scale * here, pred.shape)
    stats_in[tile, 0] = nt(centred, jnp.concatenate([centred, gap], axis=0))
    shakes = jnp.concatenate([jitter_all[i, :, lanes] for i in range(PASS_COUNT)], axis=0)
    stats_in[tile, 1] = nt(centred, shakes)
    for d in others:
        send_c(d).start()
    whole(stats_in.at[pl.ds(0, len(others))], c_send, c_recv).wait()
    total = stats_in[0]
    for d in others:
        total = total + stats_in[d]

    expand(solve(total, work), me, parts, times, mix)

    own.wait()
    step = math.gcd(256, *size)
    depth = parts * rows
    for c in range(CHUNKS):
        arrived = state.at[pl.ds(rows, depth - rows), pl.ds(first[c], size[c])]
        whole(arrived, there_send, there_recv.at[c]).wait_recv()

        def update(i, carry):
            columns = pl.ds(pl.multiple_of(first[c] + i * step, step), step)
            x = state[:, columns]
            both = jnp.dot(mix[...], x, preferred_element_type=F32)
            y = (x.astype(F32) + both[:depth] + both[depth:]).astype(BF16)
            if c < CHUNKS - 1:
                state[:, columns] = y
                column = me * (width - tail) + first[c] + i * step
                out[:, pl.ds(pl.multiple_of(column, step), step)] = y[:rows]
            else:
                last[:, aligned(i, step)] = y
                rest[:, pl.ds(pl.multiple_of(me * tail + i * step, step), step)] = y[:rows]
            return carry

        lax.fori_loop(0, size[c] // step, update, 0)
        if c < CHUNKS - 1:
            for k in partners:
                back(k, c).start()

    odd = lax.rem(me, 2) == 1

    @pl.when(odd)
    def _():
        for k in evens:
            early(k).start()

    whole(state.at[pl.ds(rows, depth - rows), :], there_send, back_recv).wait_send()
    moved = state.at[pl.ds(rows, depth - rows), pl.ds(0, width - tail)]
    whole(moved, back_send, back_recv).wait()

    @pl.when(odd)
    def _():
        whole(last.at[pl.ds(0, len(evens) * rows), :], early_send, early_recv).wait()


def finish_kernel(parts, before, last, out, send_sem, recv_sem, go_sem):
    me = lax.axis_index("mem")
    rows = out.shape[0]
    span = last.shape[1]
    partners = list(reversed(range(1, parts)))
    evens = partners[1::2]
    odds = partners[0::2]
    odd = lax.rem(me, 2) == 1
    even = jnp.logical_not(odd)
    barrier = pltpu.get_barrier_semaphore()

    def copy(k):
        return pltpu.make_async_remote_copy(
            src_ref=last.at[pl.ds(k * rows, rows), :],
            dst_ref=out.at[:, aligned(me, span)],
            send_sem=send_sem,
            recv_sem=recv_sem,
            device_id={"mem": me ^ k},
            device_id_type=MESH,
        )

    def signal(sem, k):
        pl.semaphore_signal(sem, inc=1, device_id={"mem": me ^ k}, device_id_type=MESH)

    def settle(count):
        region = last.at[pl.ds(0, count * rows), :]
        pltpu.make_async_remote_copy(
            src_ref=region,
            dst_ref=region,
            send_sem=send_sem,
            recv_sem=recv_sem,
            device_id={"mem": me ^ 1},
            device_id_type=MESH,
        ).wait()

    @pl.when(even)
    def _():
        for k in partners:
            signal(barrier, k)
        pl.semaphore_wait(barrier, len(evens))
        for k in evens:
            copy(k).start()
        pl.semaphore_wait(go_sem, len(odds))

    @pl.when(odd)
    def _():
        pl.semaphore_wait(barrier, len(odds))
        for k in odds:
            signal(go_sem, k)

    for k in odds:
        copy(k).start()

    @pl.when(odd)
    def _():
        settle(len(odds))

    @pl.when(even)
    def _():
        settle(len(partners))


def run(copies):
    for copy in copies:
        copy.start()
    for copy in copies:
        copy.wait()


def tail_piece(k, width, rest, out, sem):
    owner = lax.axis_index("mem") ^ k
    span = rest.shape[1] * width // out.shape[1]
    column = pl.multiple_of(owner * width + width - span, LANES)
    return pltpu.make_async_copy(
        rest.at[:, aligned(owner, span)], out.at[:, pl.ds(column, span)], sem.at[k]
    )


def write_most_kernel(parts, width, most, rest, out, sem, tail_sem):
    size = most.shape[1] // parts
    copies = [
        pltpu.make_async_copy(
            most.at[:, pl.ds(i * size, size)], out.at[:, pl.ds(i * width, size)], sem.at[i]
        )
        for i in range(parts)
    ]
    copies.append(tail_piece(0, width, rest, out, tail_sem))
    for copy in copies:
        copy.start()

    @pl.when(lax.rem(lax.axis_index("mem"), 2) == 1)
    def _():
        run([tail_piece(k, width, rest, out, tail_sem) for k in range(2, parts, 2)])

    for copy in copies:
        copy.wait()


def write_rest_kernel(parts, width, rest, before, out, sem):
    odd = lax.rem(lax.axis_index("mem"), 2) == 1

    @pl.when(odd)
    def _():
        run([tail_piece(k, width, rest, out, sem) for k in range(1, parts, 2)])

    @pl.when(jnp.logical_not(odd))
    def _():
        run([tail_piece(k, width, rest, out, sem) for k in range(1, parts)])


def body(prior, measured, noise, jitter, couples, target):
    parts = lax.axis_size("mem")
    tiles = lax.axis_size("pix")
    members, times, cells = prior.shape
    total_members = members * parts
    rows = members * times
    depth = rows * parts
    width = cells // parts
    obs = target.shape[0]
    unit = LANES * tiles
    padded = obs + (-obs) % unit
    share = padded // tiles
    look = LANES * BLK
    far = pl.BlockSpec(memory_space=pltpu.HBM)
    dma = pltpu.SemaphoreType.DMA
    scratch = [
        pltpu.VMEM((depth, width), BF16),
        pltpu.VMEM((2 * depth, depth), BF16),
        pltpu.VMEM((2, rows, look), BF16),
        pltpu.VMEM((look, LANES), BF16),
        pltpu.VMEM((rows, cells // BLK), F32),
        pltpu.VMEM((total_members, 2 * total_members), F32),
        pltpu.VMEM((obs,), F32),
        pltpu.VMEM((obs,), F32),
        pltpu.VMEM((2, obs), jnp.int32),
        pltpu.VMEM((obs,), jnp.int32),
        pltpu.VMEM((PASS_COUNT, total_members, obs), F32),
        pltpu.VMEM((PASS_COUNT, total_members, padded), F32),
        pltpu.VMEM((1, padded), F32),
        pltpu.VMEM((1, padded), F32),
        pltpu.VMEM((1, padded), jnp.int32),
        pltpu.VMEM((1, padded), jnp.int32),
        pltpu.VMEM((1, padded), jnp.int32),
        pltpu.VMEM((tiles, members, share), F32),
        pltpu.VMEM((tiles, members, share), F32),
        pltpu.VMEM((members, share), F32),
        pltpu.VMEM((parts, members, share), F32),
        pltpu.VMEM((tiles, 2, total_members, 2 * total_members), F32),
        dma,
        dma((CHUNKS,)),
        dma,
        dma,
        dma,
        dma,
        dma,
        dma,
        dma,
        dma,
        dma,
        dma,
        dma,
        dma,
        dma((2,)),
        dma,
        dma((5,)),
        pltpu.SemaphoreType.REGULAR,
    ]
    operands = (
        prior.reshape(rows, cells),
        measured,
        noise,
        jnp.swapaxes(jitter, 1, 2),
        couples,
        target,
    )
    span = spans(width)[-1]
    near = pl.BlockSpec(memory_space=pltpu.VMEM)
    most, rest, last = pl.pallas_call(
        functools.partial(smoother_kernel, parts, tiles, times),
        in_specs=[far] * 6,
        out_specs=[near] * 3,
        out_shape=[
            pltpu.VMEM((rows, parts * (width - span)), BF16),
            pltpu.VMEM((rows, parts * span), BF16),
            pltpu.VMEM((depth, span), BF16),
        ],
        scratch_shapes=scratch,
        compiler_params=pltpu.CompilerParams(
            collective_id=0, has_side_effects=True, vmem_limit_bytes=44 * 1024 * 1024
        ),
        name="smoother",
    )(*(pltpu.with_memory_space_constraint(a, pltpu.HBM) for a in operands))
    out = pl.pallas_call(
        functools.partial(write_most_kernel, parts, width),
        in_specs=[near, near],
        out_specs=far,
        out_shape=pltpu.HBM((rows, cells), BF16),
        scratch_shapes=[dma((parts,)), dma((parts,))],
        compiler_params=pltpu.CompilerParams(vmem_limit_bytes=4 * 1024 * 1024),
        name="write_most",
    )(most, rest)
    rest = pl.pallas_call(
        functools.partial(finish_kernel, parts),
        in_specs=[far, near],
        out_specs=near,
        out_shape=pltpu.VMEM((rows, parts * span), BF16),
        scratch_shapes=[dma, dma, pltpu.SemaphoreType.REGULAR],
        compiler_params=pltpu.CompilerParams(
            collective_id=1, has_side_effects=True, vmem_limit_bytes=8 * 1024 * 1024
        ),
        name="finish",
    )(pltpu.with_memory_space_constraint(out, pltpu.HBM), last)
    out = pl.pallas_call(
        functools.partial(write_rest_kernel, parts, width),
        in_specs=[near, far],
        out_specs=far,
        out_shape=pltpu.HBM((rows, cells), BF16),
        input_output_aliases={1: 0},
        scratch_shapes=[dma((parts,))],
        compiler_params=pltpu.CompilerParams(vmem_limit_bytes=4 * 1024 * 1024),
        name="write_rest",
    )(rest, out)
    return out.reshape(prior.shape)


def solution(mesh):
    return jax.shard_map(
        body,
        mesh=mesh,
        in_specs=(P("mem", None, "pix"), P(), P(), P(), P(), P()),
        out_specs=P("mem", None, "pix"),
        check_vma=False,
    )
```
